32 devices in a mesh: dp: 8 (over z, y), section: 2 (over core), tensor: 2 (over x).
Axes of the slice: x: 2, y: 2, z: 4, core: 2. Of those that a mesh axis runs over, the one named last changes fastest.
Arguments:
- tower_input: bfloat16 [2, 1536, 1024], P('section', 'dp'), may hold values from -8 to 8
- up_weight: bfloat16 [2, 1024, 4096], P('section', None, 'tensor'), may hold values from -0.1875 to 0.1875
- down_weight: bfloat16 [2, 4096, 1024], P('section', 'tensor'), may hold values from -0.09375 to 0.09375
- pair: int32 [1536], P('dp'), may hold values from 0 to 1535, each once
- scale: float32 [1], replicated, may hold values from 4 to 16
- bias: float32 [1], replicated, may hold values from -4 to -1
Outputs:
- loss: float32 [1], replicated
- slide_grad: float32 [1536, 1024], P(('dp', 'section', 'tensor'))
- report_grad: float32 [1536, 1024], P(('dp', 'section', 'tensor'))
The draws below stay inside these ranges and needn't reach their ends.
Inputs may be any that keep to these rules, and one draw needn't show every extreme that they name: `pair`: each report index appears exactly once.
All inputs are finite; a program needn't handle non-finite values.
Results may differ from the reference program's by a relative error of at most 0.00036.
Values may be sent and summed in bfloat16 or wider, within the bound.
A program may use at most 128 MiB of HBM per device.

```python
import math
import jax
import jax.numpy as jnp
from jax import lax

D = 1024
H = 4096
PAIRS_DEV = 48
B = 1536


def draw_tower_input(key, part):
    key_center = jax.random.fold_in(key, 11)
    key_member = jax.random.fold_in(key, 12)
    key_strength = jax.random.fold_in(key, 13)
    key_noise = jax.random.fold_in(key, 14)
    groups = 8
    centers = jax.random.normal(key_center, (groups, D), jnp.float32)
    member = jax.random.randint(key_member, (2, B), 0, groups)
    strength = jnp.exp(jax.random.uniform(key_strength, (2, B, 1), jnp.float32, jnp.log(0.4), jnp.log(1.6)))
    noise = 0.6 * jax.random.normal(key_noise, (2, B, D), jnp.float32)
    shared = jnp.take(centers, member, axis=0) * strength
    values = jnp.clip(shared + noise, -8.0, 8.0)
    return values.astype(jnp.bfloat16)


def level_of(key, shape, split, least, top_value):
    factor_of, own = 1.0, jax.random.fold_in(key, 6)
    for dim, shards_of in split:
        heights = jnp.exp(jax.random.uniform(jax.random.fold_in(own, dim), (shards_of,), jnp.float32, least / len(split), top_value / len(split)))
        factor_of = factor_of * jnp.repeat(heights, shape[dim] // shards_of).reshape([-1 if axis == dim else 1 for axis in range(len(shape))])
    return factor_of


def scatter_about(rng, extent, scale, reach, split=(), kind=jnp.bfloat16):
    result = jax.random.normal(rng, extent, jnp.float32) * scale
    if len(split) > 0:
        result = level_of(rng, extent, split, -0.22, 0.18) * result
    return jnp.clip(result, min=-reach, max=reach).astype(kind)


def setup_inputs(seed: int = 0) -> dict:
    streams_of = jax.random.split(jax.random.key(seed), 7)
    return {
        "tower_input": draw_tower_input(jax.random.fold_in(streams_of[6], 71), 0),
        "up_weight": scatter_about(streams_of[1], (2, D, H), D ** -0.5, 0.1875, ((0, 2), (2, 2))),
        "down_weight": scatter_about(streams_of[2], (2, H, D), H ** -0.5, 0.09375, ((0, 2), (1, 2))),
        "pair": jax.random.permutation(streams_of[3], B).astype(jnp.int32),
        "scale": jnp.clip(jnp.exp(jax.random.uniform(streams_of[4], (1,), jnp.float32, math.log(4.0), math.log(16.0))), 4.0, 16.0),
        "bias": jnp.clip(jax.random.uniform(streams_of[5], (1,), jnp.float32, -4.0, -1.0), -4.0, -1.0),
    }


def tower(inputs, up_part, down_part):
    hidden = jax.nn.gelu(jnp.dot(inputs, up_part, preferred_element_type=jnp.float32)).astype(jnp.bfloat16)
    raw = inputs.astype(jnp.float32) + jnp.dot(hidden, down_part, preferred_element_type=jnp.float32)
    norms = lax.rsqrt(lax.optimization_barrier(jnp.sum(raw * raw, axis=-1, keepdims=True)) + 1e-06)
    return (raw * norms).astype(jnp.bfloat16)

def reference(tower_input, up_weight, down_weight, pair, scale, bias):
    slides = tower(tower_input[0], up_weight[0], down_weight[0])
    reports = tower(tower_input[1], up_weight[1], down_weight[1])
    total = slides.shape[0]
    block = 4 * PAIRS_DEV
    columns = jnp.arange(total, dtype=jnp.int32)

    def step(carry, index):
        loss_sum, report_sum = carry
        start = (index * block).astype(jnp.int32)
        slide_rows = lax.dynamic_slice_in_dim(slides, start, block, 0)
        pair_rows = lax.dynamic_slice_in_dim(pair, start, block, 0)
        logits = scale[0] * lax.dot_general(slide_rows, reports, (((1,), (1,)), ((), ())), preferred_element_type=jnp.float32) + bias[0]
        sign = jnp.where(pair_rows[:, None] == columns[None, :], 1.0, -1.0).astype(jnp.float32)
        loss_sum = loss_sum + jnp.sum(jnp.logaddexp(jnp.float32(0.0), -sign * logits))
        weight = (-scale[0] * sign * jax.nn.sigmoid(-sign * logits)).astype(jnp.bfloat16)
        slide_part = jnp.dot(weight, reports, preferred_element_type=jnp.float32)
        report_sum = report_sum + lax.dot_general(weight, slide_rows, (((0,), (0,)), ((), ())), preferred_element_type=jnp.float32)
        return ((loss_sum, report_sum), slide_part)
    start_carry = (jnp.zeros((), jnp.float32), jnp.zeros((total, D), jnp.float32))
    (loss_sum, report_grad), slide_parts = lax.scan(step, start_carry, jnp.arange(total // block, dtype=jnp.int32))
    loss = (loss_sum / total).reshape(1)
    return (loss, slide_parts.reshape(total, D), report_grad)
```

```python
import functools

import jax
import jax.numpy as jnp
from jax import lax
from jax.experimental import pallas as pl
from jax.experimental.pallas import tpu as pltpu
from jax.sharding import PartitionSpec as P

MESH = pl.DeviceIdType.MESH
INNER = 2
PAIR = 2
UP_PARTS = 4
DOWN_PARTS = 2
N_SUB = 6
TOP = 32767.0


def events():
    hop = {"P": 0.0, "A": 2.3, "B": 2.9, "D": 5.2}
    found = [(c * 0.8 + at, "PABD".index(kind), kind, c) for kind, at in hop.items() for c in range(N_SUB)]
    return [(kind, c) for _, _, kind, c in sorted(found)]


def wait_bytes(ref, sem):
    pltpu.make_async_copy(ref, ref, sem).wait()


def iota(shape, dim):
    return lax.broadcasted_iota(jnp.int32, shape, dim)


def step_of(value, size, count):
    return sum((value >= i * size).astype(jnp.int32) for i in range(1, count))


def to_row(column, lanes=128):
    rows = column.shape[0]
    hit = iota((rows, lanes), 0) == iota((rows, lanes), 1)
    return jnp.sum(jnp.where(hit, column, 0.0), axis=0, keepdims=True)


def to_column(row, rows):
    hit = iota((rows, row.shape[1]), 0) == iota((rows, row.shape[1]), 1)
    return jnp.sum(jnp.where(hit, row, 0.0), axis=1, keepdims=True)


def to_fixed(value):
    top = jnp.maximum(jnp.max(jnp.abs(value), axis=-1, keepdims=True), 1e-30)
    fixed = jnp.round(value * (TOP / top)).astype(jnp.int32).astype(jnp.int16)
    return fixed, top * (1.0 / TOP)


def from_fixed(fixed, unit):
    return fixed.astype(jnp.int32).astype(jnp.float32) * unit


def kernel(
    dims,
    scale_ref, bias_ref, pair_ref, x_ref, up_ref, down_ref,
    loss_out, slide_out, report_out,
    xs, up, down, hid, part, fixed, fixed_in, unit, unit_in, units, pairs, left, right,
    held, other, scores, grad, sent, sent_unit, got, got_unit, twin, loss_acc, loss_row, loss_all,
    x_sem, up_sem, down_sem, part_send, part_recv, unit_send, unit_recv, pair_send, pair_recv,
    held_recv, near_send, far_send, fwd_send, core_send, other_recv,
    sent_send, sent_unit_send, got_recv, got_unit_recv, twin_send, twin_recv, loss_send, loss_recv,
):
    n_dp, n_section, n_tensor, n_half, total = dims
    quarter = xs.shape[0] // (n_section * n_tensor)
    own_rows = n_section * quarter
    rows_dp = xs.shape[0]
    d, s, x = lax.axis_index("dp"), lax.axis_index("section"), lax.axis_index("tensor")
    y, low, half = lax.rem(d, INNER), lax.rem(d // INNER, PAIR), d // (INNER * PAIR)
    n_all = n_dp * n_section * n_tensor
    me = (d * n_section + s) * n_tensor + x
    tile_blocks = 2 * PAIR
    tile_rows = tile_blocks * own_rows
    n_tiles = n_half // PAIR

    def device_of(n):
        return {
            "dp": n // (n_section * n_tensor),
            "section": lax.rem(n // n_tensor, n_section),
            "tensor": lax.rem(n, n_tensor),
        }

    def pick(t, first, second):
        return first + t * (second - first)

    def member(t, a, b, core):
        at_y, at_low, at_half = pick(t, y, a), pick(t, b, low), pick(t, half, b)
        return {
            "dp": (at_half * PAIR + at_low) * INNER + at_y, "section": core, "tensor": pick(t, a, x)
        }

    def place_of(t):
        return pick(t, x, y), pick(t, low, half), pick(t, PAIR, n_half)

    my_a, my_b, my_n = place_of(s)
    mine = my_b * 2 + my_a
    partner = {"dp": d, "section": 1 - s, "tensor": x}

    def others(count, act):
        if n_half == PAIR:
            act(1)
        else:
            def body(k, carry):
                act(k)
                return carry
            lax.fori_loop(1, count, body, 0)

    x_copies = []
    for side, t in ((0, 1 - x), (1, x)):
        for q in range(n_section):
            x_copies.append(pltpu.make_async_copy(
                x_ref.at[pl.ds(pl.multiple_of((q * n_tensor + t) * quarter, 16), quarter)],
                xs.at[pl.ds(side * own_rows + q * quarter, quarter)],
                x_sem.at[side * n_section + q],
            ))
    for c in x_copies:
        c.start()
    up_w = up.shape[1] // UP_PARTS
    down_w = down.shape[1] // DOWN_PARTS

    def up_copy(i):
        cols = pl.ds(pl.multiple_of(i * up_w, 128), up_w)
        return pltpu.make_async_copy(up_ref.at[:, cols], up.at[:, cols], up_sem.at[i])

    def down_copy(i):
        cols = pl.ds(pl.multiple_of(i * down_w, 128), down_w)
        return pltpu.make_async_copy(down_ref.at[:, cols], down.at[:, cols], down_sem.at[i])

    for i in range(UP_PARTS):
        up_copy(i).start()
    for i in range(DOWN_PARTS):
        down_copy(i).start()

    barrier = pltpu.get_barrier_semaphore()

    def greet(n, carry):
        @pl.when(n != me)
        def _():
            pl.semaphore_signal(barrier, inc=1, device_id=device_of(n), device_id_type=MESH)
        return carry

    lax.fori_loop(0, n_all, greet, 0)
    loss_acc[...] = jnp.zeros_like(loss_acc)

    def natural(lane, t):
        q = step_of(lane, quarter, n_section)
        return (q * n_tensor + t) * quarter + (lane - q * quarter)

    def order_pairs():
        column = to_column(pair_ref[...].astype(jnp.float32), rows_dp)
        lane = iota((rows_dp, rows_dp), 1)
        t = step_of(lane, own_rows, n_tensor)
        hit = iota((rows_dp, rows_dp), 0) == natural(lane - t * own_rows, t)
        pairs[low] = jnp.sum(jnp.where(hit, column, 0.0), axis=0, keepdims=True).astype(jnp.int32)

    order_pairs()

    def report_ids(index):
        block = step_of(index, own_rows, tile_blocks)
        b = step_of(block, 2, PAIR)
        home = (b * PAIR + low) * INNER + (block - 2 * b)
        return home * rows_dp + natural(index - block * own_rows, x)

    for c in x_copies:
        c.wait()

    def first(side):
        rows = pl.ds(side * own_rows, own_rows)

        def body(i, carry):
            if side == 0:
                up_copy(i).wait()
            cols = pl.ds(pl.multiple_of(i * up_w, 128), up_w)
            h = jnp.dot(xs[rows], up[:, cols], preferred_element_type=jnp.float32)
            hid[rows, cols] = jax.nn.gelu(h).astype(jnp.bfloat16)
            return carry

        lax.fori_loop(0, UP_PARTS, body, 0)

    def second(side):
        def body(i, carry):
            if side == 0:
                down_copy(i).wait()
            cols = pl.ds(pl.multiple_of(i * down_w, 128), down_w)
            part[:, cols] = jnp.dot(
                hid[side * own_rows:(side + 1) * own_rows], down[:, cols],
                preferred_element_type=jnp.float32,
            )
            return carry

        lax.fori_loop(0, DOWN_PARTS, body, 0)

    first(0)
    second(0)
    values, units_of = to_fixed(part[...])
    fixed[...] = values
    unit[...] = to_row(units_of)
    pl.semaphore_wait(barrier, n_all - 1)

    sub = own_rows // N_SUB
    across = {"dp": d, "section": s, "tensor": 1 - x}

    def part_copy(c):
        rows = pl.ds(c * sub, sub)
        return pltpu.make_async_remote_copy(
            fixed.at[rows], fixed_in.at[rows], part_send.at[c], part_recv.at[c],
            device_id=across, device_id_type=MESH,
        )

    unit_copy = pltpu.make_async_remote_copy(
        unit, unit_in, unit_send, unit_recv, device_id=across, device_id_type=MESH
    )
    unit_copy.start()
    for c in range(N_SUB):
        part_copy(c).start()
    pair_copy = pltpu.make_async_remote_copy(
        pairs.at[low], pairs.at[low], pair_send, pair_recv,
        device_id={"dp": (half * PAIR + 1 - low) * INNER + y, "section": s, "tensor": x},
        device_id_type=MESH,
    )
    pair_copy.start()

    first(1)
    second(1)
    pair_copy.wait_recv()

    @pl.when(s == 0)
    def _():
        for b in range(PAIR):
            column = to_column(pairs[b].astype(jnp.float32), rows_dp).astype(jnp.int32)
            left[b * rows_dp:(b + 1) * rows_dp] = jnp.broadcast_to(column, (rows_dp, 128))
        right[...] = report_ids(iota((1, tile_rows), 1))

    @pl.when(s != 0)
    def _():
        left[...] = report_ids(iota((tile_rows, 128), 0))
        for b in range(PAIR):
            right[:, b * rows_dp:(b + 1) * rows_dp] = pairs[b]

    unit_copy.wait_recv()
    units[...] = jnp.broadcast_to(to_column(unit_in[...], own_rows), (own_rows, 128))

    def piece(block, c):
        return held.at[block, pl.ds(c * sub, sub)]

    def held_copy(block, c, to, sem):
        return pltpu.make_async_remote_copy(
            piece(block, c), piece(block, c), sem, held_recv.at[c, block],
            device_id=to, device_id_type=MESH,
        )

    def core_copy(block, c):
        return pltpu.make_async_remote_copy(
            piece(block, c), other.at[block, pl.ds(c * sub, sub)], core_send.at[c, block],
            other_recv.at[block], device_id=partner, device_id_type=MESH,
        )

    beside = member(s, 1 - my_a, my_b, s)

    def at_b(k):
        return lax.rem(my_b + k, my_n)

    def beyond(k):
        return member(s, my_a, at_b(k), s)

    def arrived(block, c, begin):
        if begin:
            wait_bytes(piece(block, c), held_recv.at[c, block])
            core_copy(block, c).start()
        else:
            core_copy(block, c).wait_send()

    def act_on(kind, c, begin):
        run = lambda copy: copy.start() if begin else copy.wait_send()
        if kind == "P":
            if begin:
                rows = pl.ds(c * sub, sub)
                part_copy(c).wait_recv()
                theirs = from_fixed(fixed_in[rows], units[rows, 0:1])
                raw = (part[rows] + theirs) + xs[
                    pl.ds(own_rows + c * sub, sub)
                ].astype(jnp.float32)
                norms = lax.rsqrt(jnp.sum(raw * raw, axis=-1, keepdims=True) + 1e-06)
                held[mine, rows] = (raw * norms).astype(jnp.bfloat16)
            run(held_copy(mine, c, beside, near_send.at[c]))
            others(my_n, lambda k: run(held_copy(mine, c, beyond(k), far_send.at[c, k])))
            run(core_copy(mine, c))
        elif kind == "A":
            block = my_b * 2 + 1 - my_a
            arrived(block, c, begin)

            @pl.when(s == 0)
            def _():
                others(my_n, lambda k: run(held_copy(block, c, beyond(k), fwd_send.at[c, k])))
        elif kind == "B":
            def from_b(k):
                block = at_b(k) * 2 + my_a
                arrived(block, c, begin)

                @pl.when(s != 0)
                def _():
                    run(held_copy(block, c, beside, fwd_send.at[c, k]))

            others(my_n, from_b)
        else:
            others(my_n, lambda k: arrived(at_b(k) * 2 + 1 - my_a, c, begin))

    for kind, c in events():
        act_on(kind, c, True)

    def other_block(block, carry):
        wait_bytes(other.at[block], other_recv.at[block])
        return carry

    if n_half == PAIR:
        for block in range(tile_blocks):
            other_block(block, 0)
    else:
        lax.fori_loop(0, 2 * pick(s, n_half, PAIR), other_block, 0)

    scale_value, bias_value = scale_ref[0], bias_ref[0]
    width = held.shape[2]

    def score(tile):
        m_tile, t_tile = pick(s, 0, tile), pick(s, tile, 0)
        rows = held[pl.ds(m_tile * tile_blocks, tile_blocks)].reshape(tile_rows, width)
        columns = other[pl.ds(t_tile * tile_blocks, tile_blocks)].reshape(tile_rows, width)
        logits = scale_value * lax.dot_general(
            rows, columns, (((1,), (1,)), ((), ())), preferred_element_type=jnp.float32
        ) + bias_value
        shift = (1 - 2 * s) * tile * (PAIR * PAIR * INNER * rows_dp)
        for j in range(tile_rows // 128):
            lanes = slice(j * 128, (j + 1) * 128)
            sign = jnp.where(left[...] == right[:, lanes] + shift, 1.0, -1.0).astype(jnp.float32)
            u = -sign * logits[:, lanes]
            e = jnp.exp(-jnp.abs(u))
            loss_acc[...] += jnp.maximum(u, 0.0) + jnp.log1p(e)
            sigmoid = jnp.where(u >= 0, 1.0, e) / (1.0 + e)
            scores[:, lanes] = (-scale_value * sign * sigmoid).astype(jnp.bfloat16)
        return m_tile, columns

    if n_tiles > 1:
        def clear(block, carry):
            grad[block] = jnp.zeros_like(grad[block])
            return carry

        lax.fori_loop(0, 2 * my_n, clear, 0)

        def tile_step(tile, carry):
            m_tile, columns = score(tile)
            for k in range(tile_blocks):
                grad[m_tile * tile_blocks + k] += jnp.dot(
                    scores[k * own_rows:(k + 1) * own_rows], columns,
                    preferred_element_type=jnp.float32,
                )
            return carry

        lax.fori_loop(0, n_tiles, tile_step, 0)
    else:
        _, columns = score(0)

    slot = d * n_tensor + x

    def loss_copy(n):
        return pltpu.make_async_remote_copy(
            loss_row, loss_all.at[slot], loss_send, loss_recv,
            device_id=device_of(n), device_id_type=MESH,
        )

    def send_loss(n, carry):
        loss_copy(lax.rem(me + n, n_all)).start()
        return carry

    def sent_copy(block, a, b, h):
        return pltpu.make_async_remote_copy(
            sent.at[block, pl.ds(h * quarter, quarter)], got.at[s, mine], sent_send.at[block, h],
            got_recv.at[s, mine], device_id=member(s, a, b, h), device_id_type=MESH,
        )

    def sent_unit_copy(block, a, b, h):
        return pltpu.make_async_remote_copy(
            sent_unit.at[block, h], got_unit.at[s, mine], sent_unit_send.at[block, h],
            got_unit_recv.at[s, mine], device_id=member(s, a, b, h), device_id_type=MESH,
        )

    def finish_block(block):
        if n_tiles == 1:
            grad[block] = jnp.dot(
                scores[pl.ds(pl.multiple_of(block * own_rows, 16), own_rows)], columns,
                preferred_element_type=jnp.float32,
            )

    def send_block(a, k, begin):
        b = at_b(k)
        block = b * 2 + a
        if begin:
            finish_block(block)
            values, units_of = to_fixed(grad[block])
            sent[block] = values
            for h in range(n_section):
                sent_unit[block, h] = to_row(units_of[h * quarter:(h + 1) * quarter])
        for h in range(n_section):
            for copy in (sent_unit_copy(block, a, b, h), sent_copy(block, a, b, h)):
                copy.start() if begin else copy.wait_send()

    def send_all(begin):
        others(my_n, lambda k: send_block(1 - my_a, k, begin))
        others(my_n, lambda k: send_block(my_a, k, begin))
        send_block(1 - my_a, 0, begin)

    send_all(True)
    finish_block(mine)
    twin_copy = pltpu.make_async_remote_copy(
        grad.at[mine, pl.ds(pl.multiple_of((1 - s) * quarter, 16), quarter)], twin,
        twin_send, twin_recv, device_id=partner, device_id_type=MESH,
    )
    twin_copy.start()
    loss_row[...] = jnp.sum(loss_acc[...], axis=0, keepdims=True)

    @pl.when(s == 0)
    def _():
        loss_all[slot] = loss_row[...]
        lax.fori_loop(1, n_all, send_loss, 0)

    def add_got(t, a, b, out):
        block = b * 2 + a
        wait_bytes(got_unit.at[t, block], got_unit_recv.at[t, block])
        wait_bytes(got.at[t, block], got_recv.at[t, block])
        out[...] += from_fixed(got[t, block], to_column(got_unit[t, block], quarter))

    def collect(t, out):
        a, b, count = place_of(t)
        add_got(t, 1 - a, b, out)
        others(count, lambda k: add_got(t, a, lax.rem(b + k, count), out))
        others(count, lambda k: add_got(t, 1 - a, lax.rem(b + k, count), out))

    own_sum = grad[mine, pl.ds(pl.multiple_of(s * quarter, 16), quarter)]
    twin_copy.wait_recv()

    @pl.when(s == 0)
    def _():
        slide_out[...] = own_sum
        report_out[...] = twin[...]

    @pl.when(s != 0)
    def _():
        report_out[...] = own_sum
        slide_out[...] = twin[...]

    collect(0, slide_out)
    collect(1, report_out)

    for c in range(N_SUB):
        part_copy(c).wait_send()
    unit_copy.wait_send()
    pair_copy.wait_send()
    for kind, c in events():
        act_on(kind, c, False)
    send_all(False)
    twin_copy.wait_send()
    n_chips = n_dp * n_tensor

    @pl.when(s == 0)
    def _():
        wait_bytes(loss_all.at[pl.ds(0, n_all - 1)], loss_send)
        wait_bytes(loss_all.at[pl.ds(0, n_chips - 1)], loss_recv)

    @pl.when(s != 0)
    def _():
        wait_bytes(loss_all.at[pl.ds(0, n_chips)], loss_recv)

    loss_out[0] = jnp.sum(loss_all[0:n_chips]) / total


def local(tower_input, up_weight, down_weight, pair, scale, bias):
    n_dp = lax.axis_size("dp")
    n_section = lax.axis_size("section")
    n_tensor = lax.axis_size("tensor")
    inputs, up_w, down_w = tower_input[0], up_weight[0], down_weight[0]
    rows, width = inputs.shape
    hidden = up_w.shape[1]
    group = n_section * n_tensor
    quarter = rows // group
    own_rows = n_section * quarter
    total = n_dp * rows
    n_half = n_dp // (INNER * PAIR)
    blocks = 2 * n_half
    tile_rows = 2 * PAIR * own_rows

    f32, bf16, i16, i32 = jnp.float32, jnp.bfloat16, jnp.int16, jnp.int32
    vmem = pl.BlockSpec(memory_space=pltpu.VMEM)
    smem = pl.BlockSpec(memory_space=pltpu.SMEM)
    hbm = pl.BlockSpec(memory_space=pl.ANY)
    dma = pltpu.SemaphoreType.DMA
    n_all = n_dp * group
    dims = (n_dp, n_section, n_tensor, n_half, total)
    return pl.pallas_call(
        functools.partial(kernel, dims),
        out_shape=(
            jax.ShapeDtypeStruct((1,), f32),
            jax.ShapeDtypeStruct((quarter, width), f32),
            jax.ShapeDtypeStruct((quarter, width), f32),
        ),
        in_specs=[smem, smem, vmem, hbm, hbm, hbm],
        out_specs=(smem, vmem, vmem),
        scratch_shapes=[
            pltpu.VMEM((rows, width), bf16),
            pltpu.VMEM((width, hidden), bf16),
            pltpu.VMEM((hidden, width), bf16),
            pltpu.VMEM((rows, hidden), bf16),
            pltpu.VMEM((own_rows, width), f32),
            pltpu.VMEM((own_rows, width), i16),
            pltpu.VMEM((own_rows, width), i16),
            pltpu.VMEM((1, 128), f32),
            pltpu.VMEM((1, 128), f32),
            pltpu.VMEM((own_rows, 128), f32),
            pltpu.VMEM((PAIR, 1, rows), i32),
            pltpu.VMEM((tile_rows, 128), i32),
            pltpu.VMEM((1, tile_rows), i32),
            pltpu.VMEM((blocks, own_rows, width), bf16),
            pltpu.VMEM((blocks, own_rows, width), bf16),
            pltpu.VMEM((tile_rows, tile_rows), bf16),
            pltpu.VMEM((blocks, own_rows, width), f32),
            pltpu.VMEM((blocks, own_rows, width), i16),
            pltpu.VMEM((blocks, n_section, 1, 128), f32),
            pltpu.VMEM((n_section, blocks, quarter, width), i16),
            pltpu.VMEM((n_section, blocks, 1, 128), f32),
            pltpu.VMEM((quarter, width), f32),
            pltpu.VMEM((tile_rows, 128), f32),
            pltpu.VMEM((1, 128), f32),
            pltpu.VMEM((n_all, 1, 128), f32),
            dma((group,)),
            dma((UP_PARTS,)),
            dma((DOWN_PARTS,)),
            dma((N_SUB,)),
            dma((N_SUB,)),
            dma, dma, dma, dma,
            dma((N_SUB, blocks)),
            dma((N_SUB,)),
            dma((N_SUB, n_half)),
            dma((N_SUB, n_half)),
            dma((N_SUB, blocks)),
            dma((blocks,)),
            dma((blocks, n_section)),
            dma((blocks, n_section)),
            dma((n_section, blocks)),
            dma((n_section, blocks)),
            dma, dma, dma, dma,
        ],
        compiler_params=pltpu.CompilerParams(
            collective_id=0, has_side_effects=True, vmem_limit_bytes=60 * 1024 * 1024
        ),
    )(scale, bias, pair.reshape(1, rows), inputs, up_w, down_w)


def solution(mesh):
    return jax.shard_map(
        local,
        mesh=mesh,
        in_specs=(
            P("section", "dp", None),
            P("section", None, "tensor"),
            P("section", "tensor", None),
            P("dp"),
            P(),
            P(),
        ),
        out_specs=(P(), P(("dp", "section", "tensor"), None), P(("dp", "section", "tensor"), None)),
        check_vma=False,
    )
```

```python
import functools

import jax
import jax.numpy as jnp
from jax import lax
from jax.experimental import pallas as pl
from jax.experimental.pallas import tpu as pltpu
from jax.sharding import PartitionSpec as P

MESH = pl.DeviceIdType.MESH
INNER = 2
PAIR = 2
UP_PARTS = 4
DOWN_PARTS = 2
N_SUB = 6
TOP = 32767.0


TIMES = (
    {"A": (4.0, 0.40), "B": (3.9, 0.65), "D": (6.0, 0.65)},
    {"A": (4.0, 0.50), "B": (4.1, 0.55), "D": (5.5, 0.65)},
)


def events(tower):
    found = [
        (start + c * step, "ABD".index(kind), kind, c)
        for kind, (start, step) in TIMES[tower].items() for c in range(N_SUB)
    ]
    return [("P", c) for c in range(N_SUB)] + [(kind, c) for _, _, kind, c in sorted(found)]


def wait_bytes(ref, sem):
    pltpu.make_async_copy(ref, ref, sem).wait()


def iota(shape, dim):
    return lax.broadcasted_iota(jnp.int32, shape, dim)


def step_of(value, size, count):
    return sum((value >= i * size).astype(jnp.int32) for i in range(1, count))


def to_row(column, lanes=128):
    rows = column.shape[0]
    hit = iota((rows, lanes), 0) == iota((rows, lanes), 1)
    return jnp.sum(jnp.where(hit, column, 0.0), axis=0, keepdims=True)


def to_column(row, rows):
    hit = iota((rows, row.shape[1]), 0) == iota((rows, row.shape[1]), 1)
    return jnp.sum(jnp.where(hit, row, 0.0), axis=1, keepdims=True)


def to_fixed(value):
    top = jnp.maximum(jnp.max(jnp.abs(value), axis=-1, keepdims=True), 1e-30)
    fixed = jnp.round(value * (TOP / top)).astype(jnp.int32).astype(jnp.int16)
    return fixed, top * (1.0 / TOP)


def from_fixed(fixed, unit):
    return fixed.astype(jnp.int32).astype(jnp.float32) * unit


def kernel(
    dims,
    scale_ref, bias_ref, pair_ref, x_ref, up_ref, down_ref,
    loss_out, mine_out, theirs_out,
    xs, up, down, hid, part, fixed, fixed_in, unit, unit_in, units, pairs, left, right,
    held, other, scores, grad, sent, sent_unit, relay, relay_unit, got, got_unit, twin,
    loss_acc, loss_row, loss_all,
    x_sem, up_sem, down_sem, part_send, part_recv, unit_send, unit_recv, pair_send, pair_recv,
    held_recv, near_send, far_send, fwd_send, core_send, other_recv,
    sent_send, sent_unit_send, relay_recv, relay_unit_recv, got_recv, got_unit_recv,
    twin_send, twin_recv, loss_send, loss_recv,
):
    n_dp, n_section, n_tensor, n_near, total = dims
    quarter = xs.shape[0] // (n_section * n_tensor)
    own_rows = n_section * quarter
    rows_dp = xs.shape[0]
    d, s, x = lax.axis_index("dp"), lax.axis_index("section"), lax.axis_index("tensor")
    y, near, far = lax.rem(d, INNER), lax.rem(d // INNER, n_near), d // (INNER * n_near)
    n_all = n_dp * n_section * n_tensor
    me = (d * n_section + s) * n_tensor + x
    tile_blocks = 2 * PAIR
    tile_rows = tile_blocks * own_rows
    n_tiles = n_near // PAIR

    def device_of(n):
        return {
            "dp": n // (n_section * n_tensor),
            "section": lax.rem(n // n_tensor, n_section),
            "tensor": lax.rem(n, n_tensor),
        }

    def pick(t, first, second):
        return first + t * (second - first)

    def member(t, a, b, core):
        at_y, at_near, at_far = pick(t, y, a), pick(t, near, b), pick(t, b, far)
        return {
            "dp": (at_far * n_near + at_near) * INNER + at_y, "section": core,
            "tensor": pick(t, a, x),
        }

    def place_of(t):
        return pick(t, x, y), pick(t, far, near), pick(t, PAIR, n_near)

    my_a, my_b, my_n = place_of(s)
    mine = my_b * 2 + my_a
    partner = {"dp": d, "section": 1 - s, "tensor": x}

    def others(count, act):
        if n_near == PAIR:
            act(1)
        else:
            def body(k, carry):
                act(k)
                return carry
            lax.fori_loop(1, count, body, 0)

    x_copies = []
    for side, t in ((0, 1 - x), (1, x)):
        for q in range(n_section):
            x_copies.append(pltpu.make_async_copy(
                x_ref.at[pl.ds(pl.multiple_of((q * n_tensor + t) * quarter, 16), quarter)],
                xs.at[pl.ds(side * own_rows + q * quarter, quarter)],
                x_sem.at[side * n_section + q],
            ))
    for c in x_copies:
        c.start()
    up_w = up.shape[1] // UP_PARTS
    down_w = down.shape[1] // DOWN_PARTS

    def up_copy(i):
        cols = pl.ds(pl.multiple_of(i * up_w, 128), up_w)
        return pltpu.make_async_copy(up_ref.at[:, cols], up.at[:, cols], up_sem.at[i])

    def down_copy(i):
        cols = pl.ds(pl.multiple_of(i * down_w, 128), down_w)
        return pltpu.make_async_copy(down_ref.at[:, cols], down.at[:, cols], down_sem.at[i])

    for i in range(UP_PARTS):
        up_copy(i).start()
    for i in range(DOWN_PARTS):
        down_copy(i).start()

    barrier = pltpu.get_barrier_semaphore()

    def greet(n, carry):
        @pl.when(n != me)
        def _():
            pl.semaphore_signal(barrier, inc=1, device_id=device_of(n), device_id_type=MESH)
        return carry

    lax.fori_loop(0, n_all, greet, 0)
    loss_acc[...] = jnp.zeros_like(loss_acc)

    def natural(lane, t):
        q = step_of(lane, quarter, n_section)
        return (q * n_tensor + t) * quarter + (lane - q * quarter)

    def order_pairs():
        column = to_column(pair_ref[...].astype(jnp.float32), rows_dp)
        lane = iota((rows_dp, rows_dp), 1)
        t = step_of(lane, own_rows, n_tensor)
        hit = iota((rows_dp, rows_dp), 0) == natural(lane - t * own_rows, t)
        pairs[far] = jnp.sum(jnp.where(hit, column, 0.0), axis=0, keepdims=True).astype(jnp.int32)

    order_pairs()

    def report_ids(index):
        block = step_of(index, own_rows, tile_blocks)
        b = step_of(block, 2, PAIR)
        home = (far * n_near + b) * INNER + (block - 2 * b)
        return home * rows_dp + natural(index - block * own_rows, x)

    for c in x_copies:
        c.wait()

    def first(side):
        rows = pl.ds(side * own_rows, own_rows)

        def body(i, carry):
            if side == 0:
                up_copy(i).wait()
            cols = pl.ds(pl.multiple_of(i * up_w, 128), up_w)
            h = jnp.dot(xs[rows], up[:, cols], preferred_element_type=jnp.float32)
            hid[rows, cols] = jax.nn.gelu(h).astype(jnp.bfloat16)
            return carry

        lax.fori_loop(0, UP_PARTS, body, 0)

    def second(side):
        def body(i, carry):
            if side == 0:
                down_copy(i).wait()
            cols = pl.ds(pl.multiple_of(i * down_w, 128), down_w)
            part[:, cols] = jnp.dot(
                hid[side * own_rows:(side + 1) * own_rows], down[:, cols],
                preferred_element_type=jnp.float32,
            )
            return carry

        lax.fori_loop(0, DOWN_PARTS, body, 0)

    first(0)
    second(0)
    values, units_of = to_fixed(part[...])
    fixed[...] = values
    unit[...] = to_row(units_of)
    pl.semaphore_wait(barrier, n_all - 1)

    sub = own_rows // N_SUB
    across = {"dp": d, "section": s, "tensor": 1 - x}

    def part_copy(c):
        rows = pl.ds(c * sub, sub)
        return pltpu.make_async_remote_copy(
            fixed.at[rows], fixed_in.at[rows], part_send.at[c], part_recv.at[c],
            device_id=across, device_id_type=MESH,
        )

    unit_copy = pltpu.make_async_remote_copy(
        unit, unit_in, unit_send, unit_recv, device_id=across, device_id_type=MESH
    )
    unit_copy.start()
    for c in range(N_SUB):
        part_copy(c).start()
    pair_copy = pltpu.make_async_remote_copy(
        pairs.at[far], pairs.at[far], pair_send, pair_recv,
        device_id={"dp": ((1 - far) * n_near + near) * INNER + y, "section": s, "tensor": x},
        device_id_type=MESH,
    )
    pair_copy.start()

    first(1)
    second(1)
    right[...] = report_ids(iota((1, tile_rows), 1))
    pair_copy.wait_recv()
    for b in range(PAIR):
        column = to_column(pairs[b].astype(jnp.float32), rows_dp).astype(jnp.int32)
        left[b * rows_dp:(b + 1) * rows_dp] = jnp.broadcast_to(column, (rows_dp, 128))
    unit_copy.wait_recv()
    units[...] = jnp.broadcast_to(to_column(unit_in[...], own_rows), (own_rows, 128))

    def piece(block, c):
        return held.at[block, pl.ds(c * sub, sub)]

    def held_copy(block, c, to, sem):
        return pltpu.make_async_remote_copy(
            piece(block, c), piece(block, c), sem, held_recv.at[c, block],
            device_id=to, device_id_type=MESH,
        )

    def core_copy(block, c):
        return pltpu.make_async_remote_copy(
            piece(block, c), other.at[block, pl.ds(c * sub, sub)], core_send.at[c, block],
            other_recv.at[block], device_id=partner, device_id_type=MESH,
        )

    beside = member(s, 1 - my_a, my_b, s)

    def at_b(k):
        return lax.rem(my_b + k, my_n)

    def beyond(k):
        return member(s, my_a, at_b(k), s)

    def arrived(block, c, begin):
        if begin:
            wait_bytes(piece(block, c), held_recv.at[c, block])
            core_copy(block, c).start()
        else:
            core_copy(block, c).wait_send()

    def act_on(kind, c, begin):
        run = lambda copy: copy.start() if begin else copy.wait_send()
        if kind == "P":
            if begin:
                rows = pl.ds(c * sub, sub)
                part_copy(c).wait_recv()
                theirs = from_fixed(fixed_in[rows], units[rows, 0:1])
                raw = (part[rows] + theirs) + xs[
                    pl.ds(own_rows + c * sub, sub)
                ].astype(jnp.float32)
                norms = lax.rsqrt(jnp.sum(raw * raw, axis=-1, keepdims=True) + 1e-06)
                held[mine, rows] = (raw * norms).astype(jnp.bfloat16)
            others(my_n, lambda k: run(held_copy(mine, c, beyond(k), far_send.at[c, k])))
            run(held_copy(mine, c, beside, near_send.at[c]))
            run(core_copy(mine, c))
        elif kind == "A":
            arrived(my_b * 2 + 1 - my_a, c, begin)
        elif kind == "B":
            def from_b(k):
                block = at_b(k) * 2 + my_a
                if begin:
                    wait_bytes(piece(block, c), held_recv.at[c, block])
                run(held_copy(block, c, beside, fwd_send.at[c, k]))
                run(core_copy(block, c))

            others(my_n, from_b)
        else:
            others(my_n, lambda k: arrived(at_b(k) * 2 + 1 - my_a, c, begin))

    scale_value, bias_value = scale_ref[0], bias_ref[0]
    width = held.shape[2]
    slot = d * n_tensor + x

    def loss_copy(n):
        return pltpu.make_async_remote_copy(
            loss_row, loss_all.at[slot], loss_send, loss_recv,
            device_id=device_of(n), device_id_type=MESH,
        )

    def send_loss():
        loss_row[...] = jnp.sum(loss_acc[...], axis=0, keepdims=True)
        loss_all[slot] = loss_row[...]

        def body(n, carry):
            loss_copy(lax.rem(me + n, n_all)).start()
            return carry

        lax.fori_loop(1, n_all, body, 0)

    def tile_of(ref, tile):
        return ref[pl.ds(tile * tile_blocks, tile_blocks)].reshape(tile_rows, width)

    def score(tower, block, tile):
        slides, reports = (held, other) if tower == 0 else (other, held)
        logits = scale_value * lax.dot_general(
            slides[block], tile_of(reports, tile), (((1,), (1,)), ((), ())),
            preferred_element_type=jnp.float32,
        ) + bias_value
        rows = pl.ds(pl.multiple_of(block * own_rows, 16), own_rows)
        shift = tile * (PAIR * INNER * rows_dp)
        for j in range(tile_rows // 128):
            lanes = slice(j * 128, (j + 1) * 128)
            sign = jnp.where(left[rows] == right[:, lanes] + shift, 1.0, -1.0).astype(jnp.float32)
            u = -sign * logits[:, lanes]
            e = jnp.exp(-jnp.abs(u))
            if tower == 0:
                loss_acc[...] += jnp.maximum(u, 0.0) + jnp.log1p(e)
            sigmoid = jnp.where(u >= 0, 1.0, e) / (1.0 + e)
            scores[rows, lanes] = (-scale_value * sign * sigmoid).astype(jnp.bfloat16)

    def slide_terms(block, tile):
        return jnp.dot(
            scores[pl.ds(pl.multiple_of(block * own_rows, 16), own_rows)], tile_of(other, tile),
            preferred_element_type=jnp.float32,
        )

    def report_terms():
        return lax.dot_general(
            scores[...], tile_of(other, 0), (((0,), (0,)), ((), ())),
            preferred_element_type=jnp.float32,
        ).reshape(tile_blocks, own_rows, width)

    def sent_copy(block, c, target, to, sem):
        return pltpu.make_async_remote_copy(
            sent.at[block, pl.ds(c * sub, sub)], target, sent_send.at[block, c], sem,
            device_id=to, device_id_type=MESH,
        )

    def sent_unit_copy(block, h, target, to, sem):
        return pltpu.make_async_remote_copy(
            sent_unit.at[block, h], target, sent_unit_send.at[block, h], sem,
            device_id=to, device_id_type=MESH,
        )

    def owner_unit_copy(block, h, a, b):
        return sent_unit_copy(
            block, h, got_unit.at[s, my_b], member(s, a, b, h), got_unit_recv.at[s, my_b]
        )

    def owner_copy(block, c, a, b):
        per = N_SUB // n_section
        return sent_copy(
            block, c, got.at[s, my_b, pl.ds(c % per * sub, sub)], member(s, a, b, c // per),
            got_recv.at[s, my_b],
        )

    def halves_to_rows(block, units_of):
        for h in range(n_section):
            sent_unit[block, h] = to_row(units_of[h * quarter:(h + 1) * quarter])

    def send_across(k, begin):
        b = at_b(k)
        block = b * 2 + 1 - my_a
        copies = [sent_unit_copy(block, 0, relay_unit.at[b], beside, relay_unit_recv.at[b])]
        copies += [
            sent_copy(block, c, relay.at[b, pl.ds(c * sub, sub)], beside, relay_recv.at[b, c])
            for c in range(N_SUB)
        ]
        if begin:
            values, units_of = to_fixed(grad[block])
            sent[block] = values
            sent_unit[block, 0] = to_row(units_of)
        for copy in copies:
            copy.start() if begin else copy.wait_send()

    def send_beside(begin):
        block = my_b * 2 + 1 - my_a
        if begin:
            values, units_of = to_fixed(grad[block])
            sent[block] = values
            halves_to_rows(block, units_of)
        for h in range(n_section):
            copy = owner_unit_copy(block, h, 1 - my_a, my_b)
            copy.start() if begin else copy.wait_send()
        for c in range(N_SUB):
            copy = owner_copy(block, c, 1 - my_a, my_b)
            copy.start() if begin else copy.wait_send()

    def pass_on(k, begin):
        b = at_b(k)
        block = b * 2 + my_a
        if begin:
            top = jnp.max(jnp.abs(grad[block]), axis=-1, keepdims=True)
            wait_bytes(relay_unit.at[b], relay_unit_recv.at[b])
            came = to_column(relay_unit[b], own_rows)
            units_of = jnp.maximum(top, 1e-30) * (1.0 / TOP) + came
            halves_to_rows(block, units_of)
            inverse = 1.0 / units_of
        for h in range(n_section):
            copy = owner_unit_copy(block, h, my_a, b)
            copy.start() if begin else copy.wait_send()
        for c in range(N_SUB):
            if begin:
                rows = slice(c * sub, (c + 1) * sub)
                wait_bytes(relay.at[b, pl.ds(c * sub, sub)], relay_recv.at[b, c])
                value = grad[block, rows] + from_fixed(relay[b, rows], came[rows])
                sent[block, rows] = jnp.round(value * inverse[rows]).astype(jnp.int32).astype(jnp.int16)
            copy = owner_copy(block, c, my_a, b)
            copy.start() if begin else copy.wait_send()

    twin_copy = pltpu.make_async_remote_copy(
        grad.at[mine, pl.ds(pl.multiple_of((1 - s) * quarter, 16), quarter)], twin,
        twin_send, twin_recv, device_id=partner, device_id_type=MESH,
    )

    def other_block(block):
        wait_bytes(other.at[block], other_recv.at[block])

    def run_tower(tower):
        for kind, c in events(tower):
            act_on(kind, c, True)
        if n_tiles > 1:
            def wait_block(block, carry):
                other_block(block)
                return carry

            lax.fori_loop(0, 2 * (n_near if tower == 0 else PAIR), wait_block, 0)
            if tower == 0:
                grad[0:tile_blocks] = jnp.zeros_like(grad[0:tile_blocks])

            def tile_step(tile, carry):
                for k in range(tile_blocks):
                    score(tower, k, tile)
                    if tower == 0:
                        grad[k] += slide_terms(k, tile)
                if tower == 1:
                    grad[pl.ds(tile * tile_blocks, tile_blocks)] = report_terms()
                return carry

            lax.fori_loop(0, n_tiles, tile_step, 0)
            others(my_n, lambda k: send_across(k, True))
            send_beside(True)
        elif tower == 0:
            for block in range(tile_blocks):
                other_block(block)
            for block, send in (
                ((1 - my_b) * 2 + 1 - my_a, lambda: send_across(1, True)),
                (my_b * 2 + 1 - my_a, lambda: send_beside(True)),
                ((1 - my_b) * 2 + my_a, lambda: None),
                (mine, lambda: None),
            ):
                score(tower, block, 0)
                grad[block] = slide_terms(block, 0)
                send()
        else:
            for block in (
                far * 2 + x, far * 2 + 1 - x, (1 - far) * 2 + x, (1 - far) * 2 + 1 - x,
            ):
                other_block(block)
                score(tower, block, 0)
            grad[...] = report_terms()
            send_across(1, True)
            send_beside(True)
        if tower == 0:
            send_loss()
        twin_copy.start()
        others(my_n, lambda k: pass_on(k, True))

    for tower in range(n_section):
        @pl.when(s == tower)
        def _():
            run_tower(tower)

    def add_got(t, b, out):
        wait_bytes(got_unit.at[t, b], got_unit_recv.at[t, b])
        wait_bytes(got.at[t, b], got_recv.at[t, b])
        out[...] += from_fixed(got[t, b], to_column(got_unit[t, b], quarter))

    def collect(t, out):
        _, b, count = place_of(t)
        add_got(t, b, out)
        others(count, lambda k: add_got(t, lax.rem(b + k, count), out))

    mine_out[...] = grad[mine, pl.ds(pl.multiple_of(s * quarter, 16), quarter)]
    twin_copy.wait_recv()
    theirs_out[...] = twin[...]
    collect(s, mine_out)
    collect(1 - s, theirs_out)
    for c in range(N_SUB):
        part_copy(c).wait_send()
    unit_copy.wait_send()
    pair_copy.wait_send()
    for kind, c in events(0):
        act_on(kind, c, False)
    others(my_n, lambda k: send_across(k, False))
    send_beside(False)
    others(my_n, lambda k: pass_on(k, False))
    twin_copy.wait_send()
    n_chips = n_dp * n_tensor

    @pl.when(s == 0)
    def _():
        wait_bytes(loss_all.at[pl.ds(0, n_all - 1)], loss_send)
        wait_bytes(loss_all.at[pl.ds(0, n_chips - 1)], loss_recv)

    @pl.when(s != 0)
    def _():
        wait_bytes(loss_all.at[pl.ds(0, n_chips)], loss_recv)

    loss_out[0] = jnp.sum(loss_all[0:n_chips]) / total


def local(tower_input, up_weight, down_weight, pair, scale, bias):
    n_dp = lax.axis_size("dp")
    n_section = lax.axis_size("section")
    n_tensor = lax.axis_size("tensor")
    inputs, up_w, down_w = tower_input[0], up_weight[0], down_weight[0]
    rows, width = inputs.shape
    hidden = up_w.shape[1]
    group = n_section * n_tensor
    quarter = rows // group
    own_rows = n_section * quarter
    total = n_dp * rows
    n_near = n_dp // (INNER * PAIR)
    blocks = 2 * n_near
    tile_rows = 2 * PAIR * own_rows

    f32, bf16, i16, i32 = jnp.float32, jnp.bfloat16, jnp.int16, jnp.int32
    vmem = pl.BlockSpec(memory_space=pltpu.VMEM)
    smem = pl.BlockSpec(memory_space=pltpu.SMEM)
    hbm = pl.BlockSpec(memory_space=pl.ANY)
    dma = pltpu.SemaphoreType.DMA
    n_all = n_dp * group
    dims = (n_dp, n_section, n_tensor, n_near, total)
    loss, mine, theirs = pl.pallas_call(
        functools.partial(kernel, dims),
        out_shape=(
            jax.ShapeDtypeStruct((1,), f32),
            jax.ShapeDtypeStruct((quarter, width), f32),
            jax.ShapeDtypeStruct((quarter, width), f32),
        ),
        in_specs=[smem, smem, vmem, hbm, hbm, hbm],
        out_specs=(smem, vmem, vmem),
        scratch_shapes=[
            pltpu.VMEM((rows, width), bf16),
            pltpu.VMEM((width, hidden), bf16),
            pltpu.VMEM((hidden, width), bf16),
            pltpu.VMEM((rows, hidden), bf16),
            pltpu.VMEM((own_rows, width), f32),
            pltpu.VMEM((own_rows, width), i16),
            pltpu.VMEM((own_rows, width), i16),
            pltpu.VMEM((1, 128), f32),
            pltpu.VMEM((1, 128), f32),
            pltpu.VMEM((own_rows, 128), f32),
            pltpu.VMEM((PAIR, 1, rows), i32),
            pltpu.VMEM((tile_rows, 128), i32),
            pltpu.VMEM((1, tile_rows), i32),
            pltpu.VMEM((blocks, own_rows, width), bf16),
            pltpu.VMEM((blocks, own_rows, width), bf16),
            pltpu.VMEM((tile_rows, tile_rows), bf16),
            pltpu.VMEM((blocks, own_rows, width), f32),
            pltpu.VMEM((blocks, own_rows, width), i16),
            pltpu.VMEM((blocks, n_section, 1, 128), f32),
            pltpu.VMEM((n_near, own_rows, width), i16),
            pltpu.VMEM((n_near, 1, 128), f32),
            pltpu.VMEM((n_section, n_near, quarter, width), i16),
            pltpu.VMEM((n_section, n_near, 1, 128), f32),
            pltpu.VMEM((quarter, width), f32),
            pltpu.VMEM((own_rows, 128), f32),
            pltpu.VMEM((1, 128), f32),
            pltpu.VMEM((n_all, 1, 128), f32),
            dma((group,)),
            dma((UP_PARTS,)),
            dma((DOWN_PARTS,)),
            dma((N_SUB,)),
            dma((N_SUB,)),
            dma, dma, dma, dma,
            dma((N_SUB, blocks)),
            dma((N_SUB,)),
            dma((N_SUB, n_near)),
            dma((N_SUB, n_near)),
            dma((N_SUB, blocks)),
            dma((blocks,)),
            dma((blocks, N_SUB)),
            dma((blocks, n_section)),
            dma((n_near, N_SUB)),
            dma((n_near,)),
            dma((n_section, n_near)),
            dma((n_section, n_near)),
            dma, dma, dma, dma,
        ],
        compiler_params=pltpu.CompilerParams(
            collective_id=0, has_side_effects=True, vmem_limit_bytes=107 * 512 * 1024
        ),
    )(scale, bias, pair.reshape(1, rows), inputs, up_w, down_w)
    first_core = lax.axis_index("section") == 0
    return (
        loss,
        jnp.where(first_core, mine, theirs),
        jnp.where(first_core, theirs, mine),
    )


def solution(mesh):
    return jax.shard_map(
        local,
        mesh=mesh,
        in_specs=(
            P("section", "dp", None),
            P("section", None, "tensor"),
            P("section", "tensor", None),
            P("dp"),
            P(),
            P(),
        ),
        out_specs=(P(), P(("dp", "section", "tensor"), None), P(("dp", "section", "tensor"), None)),
        check_vma=False,
    )
```

```python
import functools

import jax
import jax.numpy as jnp
from jax import lax
from jax.experimental import pallas as pl
from jax.experimental.pallas import tpu as pltpu
from jax.sharding import PartitionSpec as P

MESH = pl.DeviceIdType.MESH
INNER = 2
PAIR = 2
UP_PARTS = 4
DOWN_PARTS = 2
N_SUB = 6
TOP = 32767.0


TIMES = (
    {"A": (4.0, 0.40), "B": (3.2, 0.70), "D": (5.4, 0.70)},
    {"A": (2.6, 0.50), "B": (2.7, 0.55), "D": (5.0, 0.55)},
)


def events(tower):
    found = [
        (start + c * step, "ABD".index(kind), kind, c)
        for kind, (start, step) in TIMES[tower].items() for c in range(N_SUB)
    ]
    return [("P", c) for c in range(N_SUB)] + [(kind, c) for _, _, kind, c in sorted(found)]


def wait_bytes(ref, sem):
    pltpu.make_async_copy(ref, ref, sem).wait()


def iota(shape, dim):
    return lax.broadcasted_iota(jnp.int32, shape, dim)


def step_of(value, size, count):
    return sum((value >= i * size).astype(jnp.int32) for i in range(1, count))


def to_row(column, lanes=128):
    rows = column.shape[0]
    hit = iota((rows, lanes), 0) == iota((rows, lanes), 1)
    return jnp.sum(jnp.where(hit, column, 0.0), axis=0, keepdims=True)


def to_column(row, rows):
    hit = iota((rows, row.shape[1]), 0) == iota((rows, row.shape[1]), 1)
    return jnp.sum(jnp.where(hit, row, 0.0), axis=1, keepdims=True)


def to_fixed(value):
    top = jnp.maximum(jnp.max(jnp.abs(value), axis=-1, keepdims=True), 1e-30)
    fixed = jnp.round(value * (TOP / top)).astype(jnp.int32).astype(jnp.int16)
    return fixed, top * (1.0 / TOP)


def from_fixed(fixed, unit):
    return fixed.astype(jnp.int32).astype(jnp.float32) * unit


def kernel(
    dims,
    scale_in, bias_in, pair_in, x_ref, up_ref, down_ref,
    loss_out, mine_out, theirs_out,
    xs, up, down, hid, part, fixed, fixed_in, unit, unit_in, units, pairs, left, right,
    held, other, scores, grad, sent, sent_unit, relay, relay_unit, got, got_unit, twin,
    loss_acc, loss_row, loss_all, scale_ref, bias_ref, pair_ref,
    small_sem, x_sem, up_sem, down_sem, part_send, part_recv, unit_send, unit_recv, pair_send, pair_recv,
    held_recv, near_send, far_send, fwd_send, cross_send, core_send, other_recv,
    sent_send, sent_unit_send, relay_recv, relay_unit_recv, got_recv, got_unit_recv,
    twin_send, twin_recv, loss_send, loss_recv,
):
    n_dp, n_section, n_tensor, n_near, total = dims
    quarter = xs.shape[0] // (n_section * n_tensor)
    own_rows = n_section * quarter
    rows_dp = xs.shape[0]
    d, s, x = lax.axis_index("dp"), lax.axis_index("section"), lax.axis_index("tensor")
    y, near, far = lax.rem(d, INNER), lax.rem(d // INNER, n_near), d // (INNER * n_near)
    n_all = n_dp * n_section * n_tensor
    me = (d * n_section + s) * n_tensor + x
    tile_blocks = 2 * PAIR
    tile_rows = tile_blocks * own_rows
    n_tiles = n_near // PAIR

    def device_of(n):
        return {
            "dp": n // (n_section * n_tensor),
            "section": lax.rem(n // n_tensor, n_section),
            "tensor": lax.rem(n, n_tensor),
        }

    def pick(t, first, second):
        return first + t * (second - first)

    def member(t, a, b, core):
        at_y, at_near, at_far = pick(t, y, a), pick(t, near, b), pick(t, b, far)
        return {
            "dp": (at_far * n_near + at_near) * INNER + at_y, "section": core,
            "tensor": pick(t, a, x),
        }

    def place_of(t):
        return pick(t, x, y), pick(t, far, near), pick(t, PAIR, n_near)

    my_a, my_b, my_n = place_of(s)
    def block_of(a, b):
        return (b // PAIR) * tile_blocks + a * PAIR + lax.rem(b, PAIR)

    mine = block_of(my_a, my_b)
    partner = {"dp": d, "section": 1 - s, "tensor": x}

    def others(count, act):
        if n_near == PAIR:
            act(1)
        else:
            def body(k, carry):
                act(k)
                return carry
            lax.fori_loop(1, count, body, 0)

    x_copies = []
    for side, t in ((0, 1 - x), (1, x)):
        for q in range(n_section):
            x_copies.append(pltpu.make_async_copy(
                x_ref.at[pl.ds(pl.multiple_of((q * n_tensor + t) * quarter, 16), quarter)],
                xs.at[pl.ds(side * own_rows + q * quarter, quarter)],
                x_sem.at[side * n_section + q],
            ))
    small_copies = [
        pltpu.make_async_copy(here, there, small_sem.at[i])
        for i, (here, there) in enumerate(
            ((pair_in, pair_ref), (scale_in, scale_ref), (bias_in, bias_ref))
        )
    ]
    for c in small_copies:
        c.start()
    for c in x_copies:
        c.start()
    up_w = up.shape[1] // UP_PARTS
    down_w = down.shape[1] // DOWN_PARTS

    def up_copy(i):
        cols = pl.ds(i * up_w, up_w)
        return pltpu.make_async_copy(up_ref.at[:, cols], up.at[:, cols], up_sem.at[i])

    def down_copy(i):
        cols = pl.ds(i * down_w, down_w)
        return pltpu.make_async_copy(down_ref.at[:, cols], down.at[:, cols], down_sem.at[i])

    for i in range(UP_PARTS):
        up_copy(i).start()
    for i in range(DOWN_PARTS):
        down_copy(i).start()

    barrier = pltpu.get_barrier_semaphore()

    def greet(n, carry):
        @pl.when(n != me)
        def _():
            pl.semaphore_signal(barrier, inc=1, device_id=device_of(n), device_id_type=MESH)
        return carry

    lax.fori_loop(0, n_all, greet, 0)
    loss_acc[...] = jnp.zeros_like(loss_acc)

    def natural(lane, t):
        q = step_of(lane, quarter, n_section)
        return (q * n_tensor + t) * quarter + (lane - q * quarter)

    def order_pairs():
        column = to_column(pair_ref[...].astype(jnp.float32), rows_dp)
        lane = iota((rows_dp, rows_dp), 1)
        t = step_of(lane, own_rows, n_tensor)
        hit = iota((rows_dp, rows_dp), 0) == natural(lane - t * own_rows, t)
        pairs[far] = jnp.sum(jnp.where(hit, column, 0.0), axis=0, keepdims=True).astype(jnp.int32)

    for c in small_copies:
        c.wait()
    order_pairs()

    def report_ids(index):
        block = step_of(index, own_rows, tile_blocks)
        a = step_of(block, PAIR, 2)
        home = (far * n_near + block - PAIR * a) * INNER + a
        return home * rows_dp + natural(index - block * own_rows, x)

    for c in x_copies:
        c.wait()

    def first(side):
        rows = pl.ds(side * own_rows, own_rows)

        def body(i, carry):
            if side == 0:
                up_copy(i).wait()
            cols = pl.ds(i * up_w, up_w)
            h = jnp.dot(xs[rows], up[:, cols], preferred_element_type=jnp.float32)
            hid[rows, cols] = jax.nn.gelu(h).astype(jnp.bfloat16)
            return carry

        for i in range(UP_PARTS):
            body(i, 0)

    def second(side):
        def body(i, carry):
            if side == 0:
                down_copy(i).wait()
            cols = pl.ds(i * down_w, down_w)
            part[:, cols] = jnp.dot(
                hid[side * own_rows:(side + 1) * own_rows], down[:, cols],
                preferred_element_type=jnp.float32,
            )
            return carry

        for i in range(DOWN_PARTS):
            body(i, 0)

    first(0)
    second(0)
    values, units_of = to_fixed(part[...])
    fixed[...] = values
    unit[...] = to_row(units_of)
    pl.semaphore_wait(barrier, n_all - 1)

    sub = own_rows // N_SUB
    across = {"dp": d, "section": s, "tensor": 1 - x}

    def part_copy(c):
        rows = pl.ds(c * sub, sub)
        return pltpu.make_async_remote_copy(
            fixed.at[rows], fixed_in.at[rows], part_send.at[c], part_recv.at[c],
            device_id=across, device_id_type=MESH,
        )

    unit_copy = pltpu.make_async_remote_copy(
        unit, unit_in, unit_send, unit_recv, device_id=across, device_id_type=MESH
    )

    def send_parts():
        unit_copy.start()
        for c in range(N_SUB):
            part_copy(c).start()

    @pl.when(s == 0)
    def _():
        send_parts()

    pair_copy = pltpu.make_async_remote_copy(
        pairs.at[far], pairs.at[far], pair_send, pair_recv,
        device_id={"dp": ((1 - far) * n_near + near) * INNER + y, "section": s, "tensor": x},
        device_id_type=MESH,
    )
    pair_copy.start()

    first(1)
    second(1)

    @pl.when(s == 1)
    def _():
        send_parts()

    unit_copy.wait_recv()
    units[...] = jnp.broadcast_to(to_column(unit_in[...], own_rows), (own_rows, 128))

    def piece(block, c):
        return held.at[block, pl.ds(c * sub, sub)]

    def held_copy(block, c, to, sem):
        return pltpu.make_async_remote_copy(
            piece(block, c), piece(block, c), sem, held_recv.at[c, block],
            device_id=to, device_id_type=MESH,
        )

    def core_copy(block, c):
        return pltpu.make_async_remote_copy(
            piece(block, c), other.at[block, pl.ds(c * sub, sub)], core_send.at[c, block],
            other_recv.at[block], device_id=partner, device_id_type=MESH,
        )

    beside = member(s, 1 - my_a, my_b, s)
    beside_partner = member(s, 1 - my_a, my_b, 1 - s)

    def cross_copy(block, c, sem):
        return pltpu.make_async_remote_copy(
            piece(block, c), other.at[block, pl.ds(c * sub, sub)], sem, other_recv.at[block],
            device_id=beside_partner, device_id_type=MESH,
        )

    def at_b(k):
        return lax.rem(my_b + k, my_n)

    def beyond(k):
        return member(s, my_a, at_b(k), s)

    def arrived(block, c, begin):
        if begin:
            wait_bytes(piece(block, c), held_recv.at[c, block])
            core_copy(block, c).start()
        else:
            core_copy(block, c).wait_send()

    def act_on(kind, c, begin):
        run = lambda copy: copy.start() if begin else copy.wait_send()
        if kind == "P":
            if begin:
                rows = pl.ds(c * sub, sub)
                part_copy(c).wait_recv()
                theirs = from_fixed(fixed_in[rows], units[rows, 0:1])
                raw = (part[rows] + theirs) + xs[
                    pl.ds(own_rows + c * sub, sub)
                ].astype(jnp.float32)
                norms = lax.rsqrt(jnp.sum(raw * raw, axis=-1, keepdims=True) + 1e-06)
                held[mine, rows] = (raw * norms).astype(jnp.bfloat16)
            others(my_n, lambda k: run(held_copy(mine, c, beyond(k), far_send.at[c, k])))
            run(held_copy(mine, c, beside, near_send.at[c]))
            run(core_copy(mine, c))
        elif kind == "A":
            arrived(block_of(1 - my_a, my_b), c, begin)
        elif kind == "B":
            def from_b(k):
                block = block_of(my_a, at_b(k))
                if begin:
                    wait_bytes(piece(block, c), held_recv.at[c, block])
                run(cross_copy(block, c, cross_send.at[c, k]))
                run(held_copy(block, c, beside, fwd_send.at[c, k]))
                run(core_copy(block, c))

            others(my_n, from_b)
        elif begin:
            def from_both(k):
                block = block_of(1 - my_a, at_b(k))
                wait_bytes(piece(block, c), held_recv.at[c, block])

            others(my_n, from_both)

    scale_value, bias_value = scale_ref[...], bias_ref[...]
    width = held.shape[2]
    slot = d * n_tensor + x

    def loss_copy(n):
        return pltpu.make_async_remote_copy(
            loss_row, loss_all.at[slot], loss_send, loss_recv,
            device_id=device_of(n), device_id_type=MESH,
        )

    def send_loss():
        loss_row[...] = jnp.sum(loss_acc[...], axis=0, keepdims=True)
        loss_all[slot] = loss_row[...]

        def body(n, carry):
            loss_copy(lax.rem(me + n, n_all)).start()
            return carry

        lax.fori_loop(1, n_all, body, 0)

    def tile_of(ref, tile):
        return ref[pl.ds(tile * tile_blocks, tile_blocks)].reshape(tile_rows, width)

    def score(tower, a, tile):
        slides, reports = (held, other) if tower == 0 else (other, held)
        logits = scale_value * lax.dot_general(
            slides[pl.ds(a * PAIR, PAIR)].reshape(rows_dp, width), tile_of(reports, tile),
            (((1,), (1,)), ((), ())), preferred_element_type=jnp.float32,
        ) + bias_value
        rows = pl.ds(pl.multiple_of(a * rows_dp, 16), rows_dp)
        shift = tile * (PAIR * INNER * rows_dp)
        for j in range(tile_rows // 128):
            lanes = slice(j * 128, (j + 1) * 128)
            sign = jnp.where(left[rows] == right[:, lanes] + shift, 1.0, -1.0).astype(jnp.float32)
            u = -sign * logits[:, lanes]
            e = jnp.exp(-jnp.abs(u))
            if tower == 1:
                loss_acc[...] += jnp.maximum(u, 0.0) + jnp.log1p(e)
            sigmoid = jnp.where(u >= 0, 1.0, e) / (1.0 + e)
            scores[rows, lanes] = (-scale_value * sign * sigmoid).astype(jnp.bfloat16)

    def slide_terms(a, tile):
        return jnp.dot(
            scores[pl.ds(pl.multiple_of(a * rows_dp, 16), rows_dp)], tile_of(other, tile),
            preferred_element_type=jnp.float32,
        ).reshape(PAIR, own_rows, width)

    def report_terms():
        return lax.dot_general(
            scores[...], tile_of(other, 0), (((0,), (0,)), ((), ())),
            preferred_element_type=jnp.float32,
        ).reshape(tile_blocks, own_rows, width)

    def sent_copy(block, c, target, to, sem):
        return pltpu.make_async_remote_copy(
            sent.at[block, pl.ds(c * sub, sub)], target, sent_send.at[block, c], sem,
            device_id=to, device_id_type=MESH,
        )

    def sent_unit_copy(block, h, target, to, sem):
        return pltpu.make_async_remote_copy(
            sent_unit.at[block, h], target, sent_unit_send.at[block, h], sem,
            device_id=to, device_id_type=MESH,
        )

    def owner_unit_copy(block, h, a, b):
        return sent_unit_copy(
            block, h, got_unit.at[s, my_b], member(s, a, b, h), got_unit_recv.at[s, my_b]
        )

    def owner_copy(block, c, a, b):
        per = N_SUB // n_section
        return sent_copy(
            block, c, got.at[s, my_b, pl.ds(c % per * sub, sub)], member(s, a, b, c // per),
            got_recv.at[s, my_b],
        )

    def halves_to_rows(block, units_of):
        for h in range(n_section):
            sent_unit[block, h] = to_row(units_of[h * quarter:(h + 1) * quarter])

    def send_across(k, begin):
        b = at_b(k)
        block = block_of(1 - my_a, b)
        copies = [sent_unit_copy(block, 0, relay_unit.at[b], beside, relay_unit_recv.at[b])]
        copies += [
            sent_copy(block, c, relay.at[b, pl.ds(c * sub, sub)], beside, relay_recv.at[b, c])
            for c in range(N_SUB)
        ]
        if begin:
            values, units_of = to_fixed(grad[block])
            sent[block] = values
            sent_unit[block, 0] = to_row(units_of)
        for copy in copies:
            copy.start() if begin else copy.wait_send()

    def send_beside(begin):
        block = block_of(1 - my_a, my_b)
        if begin:
            values, units_of = to_fixed(grad[block])
            sent[block] = values
            halves_to_rows(block, units_of)
        for h in range(n_section):
            copy = owner_unit_copy(block, h, 1 - my_a, my_b)
            copy.start() if begin else copy.wait_send()
        for c in range(N_SUB):
            copy = owner_copy(block, c, 1 - my_a, my_b)
            copy.start() if begin else copy.wait_send()

    def pass_on(k, begin):
        b = at_b(k)
        block = block_of(my_a, b)
        if begin:
            top = jnp.max(jnp.abs(grad[block]), axis=-1, keepdims=True)
            wait_bytes(relay_unit.at[b], relay_unit_recv.at[b])
            came = to_column(relay_unit[b], own_rows)
            units_of = jnp.maximum(top, 1e-30) * (1.0 / TOP) + came
            halves_to_rows(block, units_of)
            inverse = 1.0 / units_of
        for h in range(n_section):
            copy = owner_unit_copy(block, h, my_a, b)
            copy.start() if begin else copy.wait_send()
        for c in range(N_SUB):
            if begin:
                rows = slice(c * sub, (c + 1) * sub)
                wait_bytes(relay.at[b, pl.ds(c * sub, sub)], relay_recv.at[b, c])
                value = grad[block, rows] + from_fixed(relay[b, rows], came[rows])
                sent[block, rows] = jnp.round(value * inverse[rows]).astype(jnp.int32).astype(jnp.int16)
            copy = owner_copy(block, c, my_a, b)
            copy.start() if begin else copy.wait_send()

    twin_copy = pltpu.make_async_remote_copy(
        grad.at[mine, pl.ds(pl.multiple_of((1 - s) * quarter, 16), quarter)], twin,
        twin_send, twin_recv, device_id=partner, device_id_type=MESH,
    )

    def other_block(block):
        wait_bytes(other.at[block], other_recv.at[block])

    def make_ids():
        right[...] = report_ids(iota((1, tile_rows), 1))
        pair_copy.wait_recv()
        for b in range(PAIR):
            column = to_column(pairs[b].astype(jnp.float32), rows_dp).astype(jnp.int32)
            for a in range(n_tensor):
                at = (a * PAIR + b) * own_rows
                left[at:at + own_rows] = jnp.broadcast_to(
                    column[a * own_rows:(a + 1) * own_rows], (own_rows, 128)
                )

    def run_tower(tower):
        for kind, c in events(tower):
            act_on(kind, c, True)
            if (kind, c) == ("P", N_SUB - 1):
                make_ids()
        if n_tiles > 1:
            def wait_block(block, carry):
                other_block(block)
                return carry

            lax.fori_loop(0, 2 * (n_near if tower == 0 else PAIR), wait_block, 0)
            if tower == 0:
                grad[0:tile_blocks] = jnp.zeros_like(grad[0:tile_blocks])

            def tile_step(tile, carry):
                for a in range(2):
                    score(tower, a, tile)
                    if tower == 0:
                        grad[a * PAIR:(a + 1) * PAIR] += slide_terms(a, tile)
                if tower == 1:
                    grad[pl.ds(tile * tile_blocks, tile_blocks)] = report_terms()
                return carry

            lax.fori_loop(0, n_tiles, tile_step, 0)
            others(my_n, lambda k: send_across(k, True))
            send_beside(True)
        elif tower == 0:
            for block in range(tile_blocks):
                other_block(block)
            score(tower, 1 - my_a, 0)
            grad[pl.ds((1 - my_a) * PAIR, PAIR)] = slide_terms(1 - my_a, 0)
            send_across(1, True)
            send_beside(True)
            score(tower, my_a, 0)
            grad[pl.ds(my_a * PAIR, PAIR)] = slide_terms(my_a, 0)
        else:
            for a in (x, 1 - x):
                for b in (far, 1 - far):
                    other_block(block_of(a, b))
                score(tower, a, 0)
            grad[...] = report_terms()
            send_across(1, True)
            send_beside(True)
        if tower == 1:
            send_loss()
        twin_copy.start()
        others(my_n, lambda k: pass_on(k, True))

    for tower in range(n_section):
        @pl.when(s == tower)
        def _():
            run_tower(tower)

    def add_got(t, b, out):
        wait_bytes(got_unit.at[t, b], got_unit_recv.at[t, b])
        wait_bytes(got.at[t, b], got_recv.at[t, b])
        out[...] += from_fixed(got[t, b], to_column(got_unit[t, b], quarter))

    def collect(t, out):
        _, b, count = place_of(t)
        add_got(t, b, out)
        others(count, lambda k: add_got(t, lax.rem(b + k, count), out))

    mine_out[...] = grad[mine, pl.ds(pl.multiple_of(s * quarter, 16), quarter)]
    twin_copy.wait_recv()
    theirs_out[...] = twin[...]
    collect(s, mine_out)
    collect(1 - s, theirs_out)
    for c in range(N_SUB):
        part_copy(c).wait_send()
    unit_copy.wait_send()
    pair_copy.wait_send()
    for kind, c in events(0):
        act_on(kind, c, False)
    others(my_n, lambda k: send_across(k, False))
    send_beside(False)
    others(my_n, lambda k: pass_on(k, False))
    twin_copy.wait_send()
    n_chips = n_dp * n_tensor

    @pl.when(s == 1)
    def _():
        wait_bytes(loss_all.at[pl.ds(0, n_all - 1)], loss_send)
        wait_bytes(loss_all.at[pl.ds(0, n_chips - 1)], loss_recv)

    @pl.when(s != 1)
    def _():
        wait_bytes(loss_all.at[pl.ds(0, n_chips)], loss_recv)

    loss_out[...] = jnp.broadcast_to(jnp.sum(loss_all[0:n_chips]) / total, loss_out.shape)


def local(tower_input, up_weight, down_weight, pair, scale, bias):
    n_dp = lax.axis_size("dp")
    n_section = lax.axis_size("section")
    n_tensor = lax.axis_size("tensor")
    inputs, up_w, down_w = tower_input[0], up_weight[0], down_weight[0]
    rows, width = inputs.shape
    hidden = up_w.shape[1]
    group = n_section * n_tensor
    quarter = rows // group
    own_rows = n_section * quarter
    total = n_dp * rows
    n_near = n_dp // (INNER * PAIR)
    blocks = 2 * n_near
    tile_rows = 2 * PAIR * own_rows

    f32, bf16, i16, i32 = jnp.float32, jnp.bfloat16, jnp.int16, jnp.int32
    vmem = pl.BlockSpec(memory_space=pltpu.VMEM)
    hbm = pl.BlockSpec(memory_space=pl.ANY)
    dma = pltpu.SemaphoreType.DMA
    n_all = n_dp * group
    dims = (n_dp, n_section, n_tensor, n_near, total)
    loss, mine, theirs = pl.pallas_call(
        functools.partial(kernel, dims),
        out_shape=(
            jax.ShapeDtypeStruct((1, 128), f32),
            jax.ShapeDtypeStruct((quarter, width), f32),
            jax.ShapeDtypeStruct((quarter, width), f32),
        ),
        in_specs=[hbm] * 6,
        out_specs=(vmem, vmem, vmem),
        scratch_shapes=[
            pltpu.VMEM((rows, width), bf16),
            pltpu.VMEM((width, hidden), bf16),
            pltpu.VMEM((hidden, width), bf16),
            pltpu.VMEM((rows, hidden), bf16),
            pltpu.VMEM((own_rows, width), f32),
            pltpu.VMEM((own_rows, width), i16),
            pltpu.VMEM((own_rows, width), i16),
            pltpu.VMEM((1, 128), f32),
            pltpu.VMEM((1, 128), f32),
            pltpu.VMEM((own_rows, 128), f32),
            pltpu.VMEM((PAIR, 1, rows), i32),
            pltpu.VMEM((tile_rows, 128), i32),
            pltpu.VMEM((1, tile_rows), i32),
            pltpu.VMEM((blocks, own_rows, width), bf16),
            pltpu.VMEM((blocks, own_rows, width), bf16),
            pltpu.VMEM((tile_rows, tile_rows), bf16),
            pltpu.VMEM((blocks, own_rows, width), f32),
            pltpu.VMEM((blocks, own_rows, width), i16),
            pltpu.VMEM((blocks, n_section, 1, 128), f32),
            pltpu.VMEM((n_near, own_rows, width), i16),
            pltpu.VMEM((n_near, 1, 128), f32),
            pltpu.VMEM((n_section, n_near, quarter, width), i16),
            pltpu.VMEM((n_section, n_near, 1, 128), f32),
            pltpu.VMEM((quarter, width), f32),
            pltpu.VMEM((rows, 128), f32),
            pltpu.VMEM((1, 128), f32),
            pltpu.VMEM((n_all, 1, 128), f32),
            pltpu.VMEM((1, 1), f32),
            pltpu.VMEM((1, 1), f32),
            pltpu.VMEM((1, rows), i32),
            dma((3,)),
            dma((group,)),
            dma((UP_PARTS,)),
            dma((DOWN_PARTS,)),
            dma((N_SUB,)),
            dma((N_SUB,)),
            dma, dma, dma, dma,
            dma((N_SUB, blocks)),
            dma((N_SUB,)),
            dma((N_SUB, n_near)),
            dma((N_SUB, n_near)),
            dma((N_SUB, n_near)),
            dma((N_SUB, blocks)),
            dma((blocks,)),
            dma((blocks, N_SUB)),
            dma((blocks, n_section)),
            dma((n_near, N_SUB)),
            dma((n_near,)),
            dma((n_section, n_near)),
            dma((n_section, n_near)),
            dma, dma, dma, dma,
        ],
        compiler_params=pltpu.CompilerParams(
            collective_id=0, has_side_effects=True, vmem_limit_bytes=52 * 1024 * 1024
        ),
    )(scale.reshape(1, 1), bias.reshape(1, 1), *(
        pltpu.with_memory_space_constraint(a, pltpu.HBM)
        for a in (pair.reshape(1, rows), inputs, up_w, down_w)
    ))
    first_core = lax.axis_index("section") == 0
    return (
        loss[0, :1],
        jnp.where(first_core, mine, theirs),
        jnp.where(first_core, theirs, mine),
    )


def solution(mesh):
    return jax.shard_map(
        local,
        mesh=mesh,
        in_specs=(
            P("section", "dp", None),
            P("section", None, "tensor"),
            P("section", "tensor", None),
            P("dp"),
            P(),
            P(),
        ),
        out_specs=(P(), P(("dp", "section", "tensor"), None), P(("dp", "section", "tensor"), None)),
        check_vma=False,
    )
```

```python
import functools

import jax
import jax.numpy as jnp
from jax import lax
from jax.experimental import pallas as pl
from jax.experimental.pallas import tpu as pltpu
from jax.sharding import PartitionSpec as P

MESH = pl.DeviceIdType.MESH
INNER = 2
PAIR = 2
UP_PARTS = 2
DOWN_PARTS = 1
N_SUB = 6
R_SUB = 6
TOP = 32767.0


TIMES = (
    {"A": (4.0, 0.40), "B": (3.2, 0.70), "D": (5.4, 0.70)},
    {"A": (2.6, 0.50), "B": (2.7, 0.55), "D": (5.0, 0.55)},
)


def events(tower):
    found = [
        (start + c * step, "ABD".index(kind), kind, c)
        for kind, (start, step) in TIMES[tower].items() for c in range(N_SUB)
    ]
    return [("P", c) for c in range(N_SUB)] + [(kind, c) for _, _, kind, c in sorted(found)]


def wait_bytes(ref, sem):
    pltpu.make_async_copy(ref, ref, sem).wait()


def iota(shape, dim):
    return lax.broadcasted_iota(jnp.int32, shape, dim)


def step_of(value, size, count):
    return sum((value >= i * size).astype(jnp.int32) for i in range(1, count))


def to_row(column, lanes=128):
    rows = column.shape[0]
    hit = iota((rows, lanes), 0) == iota((rows, lanes), 1)
    return jnp.sum(jnp.where(hit, column, 0.0), axis=0, keepdims=True)


def to_column(row, rows):
    hit = iota((rows, row.shape[1]), 0) == iota((rows, row.shape[1]), 1)
    return jnp.sum(jnp.where(hit, row, 0.0), axis=1, keepdims=True)


def to_fixed(value):
    top = jnp.maximum(jnp.max(jnp.abs(value), axis=-1, keepdims=True), 1e-30)
    fixed = jnp.round(value * (TOP / top)).astype(jnp.int32).astype(jnp.int16)
    return fixed, top * (1.0 / TOP)


def from_fixed(fixed, unit):
    return fixed.astype(jnp.int32).astype(jnp.float32) * unit


def kernel(
    dims,
    scale_in, bias_in, pair_in, x_ref, up_ref, down_ref,
    loss_out, mine_out, theirs_out,
    xs, up, down, hid, part, fixed, fixed_in, unit, unit_in, units, pairs, left, right,
    held, other, scores, grad, sent, sent_unit, relay, relay_unit, got, got_unit, twin,
    loss_acc, loss_row, loss_all, scale_ref, bias_ref, pair_ref,
    small_sem, x_sem, up_sem, down_sem, part_send, part_recv, unit_send, unit_recv, pair_send, pair_recv,
    held_recv, near_send, far_send, fwd_send, cross_send, core_send, other_recv,
    sent_send, sent_unit_send, relay_recv, relay_unit_recv, got_recv, got_unit_recv,
    twin_send, twin_recv, loss_send, loss_recv,
):
    n_dp, n_section, n_tensor, n_near, total = dims
    quarter = xs.shape[0] // (n_section * n_tensor)
    own_rows = n_section * quarter
    rows_dp = xs.shape[0]
    d, s, x = lax.axis_index("dp"), lax.axis_index("section"), lax.axis_index("tensor")
    y, near, far = lax.rem(d, INNER), lax.rem(d // INNER, n_near), d // (INNER * n_near)
    n_all = n_dp * n_section * n_tensor
    me = (d * n_section + s) * n_tensor + x
    tile_blocks = 2 * PAIR
    tile_rows = tile_blocks * own_rows
    n_tiles = n_near // PAIR

    def device_of(n):
        return {
            "dp": n // (n_section * n_tensor),
            "section": lax.rem(n // n_tensor, n_section),
            "tensor": lax.rem(n, n_tensor),
        }

    def pick(t, first, second):
        return first + t * (second - first)

    def member(t, a, b, core):
        at_y, at_near, at_far = pick(t, y, a), pick(t, near, b), pick(t, b, far)
        return {
            "dp": (at_far * n_near + at_near) * INNER + at_y, "section": core,
            "tensor": pick(t, a, x),
        }

    def place_of(t):
        return pick(t, x, y), pick(t, far, near), pick(t, PAIR, n_near)

    my_a, my_b, my_n = place_of(s)
    def block_of(a, b):
        return (b // PAIR) * tile_blocks + a * PAIR + lax.rem(b, PAIR)

    mine = block_of(my_a, my_b)
    partner = {"dp": d, "section": 1 - s, "tensor": x}

    def others(count, act):
        if n_near == PAIR:
            act(1)
        else:
            def body(k, carry):
                act(k)
                return carry
            lax.fori_loop(1, count, body, 0)

    x_copies = []
    for side, t in ((0, 1 - x), (1, x)):
        for q in range(n_section):
            x_copies.append(pltpu.make_async_copy(
                x_ref.at[pl.ds(pl.multiple_of((q * n_tensor + t) * quarter, 16), quarter)],
                xs.at[pl.ds(side * own_rows + q * quarter, quarter)],
                x_sem.at[side * n_section + q],
            ))
    small_copies = [
        pltpu.make_async_copy(here, there, small_sem.at[i])
        for i, (here, there) in enumerate(
            ((pair_in, pair_ref), (scale_in, scale_ref), (bias_in, bias_ref))
        )
    ]
    for c in small_copies:
        c.start()
    for c in x_copies:
        c.start()
    up_w = up.shape[1] // UP_PARTS
    down_w = down.shape[1] // DOWN_PARTS

    def up_copy(i):
        cols = pl.ds(i * up_w, up_w)
        return pltpu.make_async_copy(up_ref.at[:, cols], up.at[:, cols], up_sem.at[i])

    def down_copy(i):
        cols = pl.ds(i * down_w, down_w)
        return pltpu.make_async_copy(down_ref.at[:, cols], down.at[:, cols], down_sem.at[i])

    for i in range(UP_PARTS):
        up_copy(i).start()
    for i in range(DOWN_PARTS):
        down_copy(i).start()

    barrier = pltpu.get_barrier_semaphore()

    def greet(n, carry):
        @pl.when(n != me)
        def _():
            pl.semaphore_signal(barrier, inc=1, device_id=device_of(n), device_id_type=MESH)
        return carry

    lax.fori_loop(0, n_all, greet, 0)
    loss_acc[...] = jnp.zeros_like(loss_acc)

    def natural(lane, t):
        q = step_of(lane, quarter, n_section)
        return (q * n_tensor + t) * quarter + (lane - q * quarter)

    def order_pairs():
        column = to_column(pair_ref[...].astype(jnp.float32), rows_dp)
        lane = iota((rows_dp, rows_dp), 1)
        t = step_of(lane, own_rows, n_tensor)
        hit = iota((rows_dp, rows_dp), 0) == natural(lane - t * own_rows, t)
        pairs[far] = jnp.sum(jnp.where(hit, column, 0.0), axis=0, keepdims=True).astype(jnp.int32)

    for c in small_copies:
        c.wait()
    order_pairs()

    def report_ids(index):
        block = step_of(index, own_rows, tile_blocks)
        a = step_of(block, PAIR, 2)
        home = (far * n_near + block - PAIR * a) * INNER + a
        return home * rows_dp + natural(index - block * own_rows, x)

    for c in x_copies:
        c.wait()

    def first(side):
        rows = pl.ds(side * own_rows, own_rows)

        def body(i, carry):
            if side == 0:
                up_copy(i).wait()
            cols = pl.ds(i * up_w, up_w)
            h = jnp.dot(xs[rows], up[:, cols], preferred_element_type=jnp.float32)
            hid[rows, cols] = jax.nn.gelu(h).astype(jnp.bfloat16)
            return carry

        for i in range(UP_PARTS):
            body(i, 0)

    def second(side):
        def body(i, carry):
            if side == 0:
                down_copy(i).wait()
            cols = pl.ds(i * down_w, down_w)
            part[:, cols] = jnp.dot(
                hid[side * own_rows:(side + 1) * own_rows], down[:, cols],
                preferred_element_type=jnp.float32,
            )
            return carry

        for i in range(DOWN_PARTS):
            body(i, 0)

    first(0)
    second(0)
    values, units_of = to_fixed(part[...])
    fixed[...] = values
    unit[...] = to_row(units_of)
    pl.semaphore_wait(barrier, n_all - 1)

    sub = own_rows // N_SUB
    across = {"dp": d, "section": s, "tensor": 1 - x}

    def part_copy(c):
        rows = pl.ds(c * sub, sub)
        return pltpu.make_async_remote_copy(
            fixed.at[rows], fixed_in.at[rows], part_send.at[c], part_recv.at[c],
            device_id=across, device_id_type=MESH,
        )

    unit_copy = pltpu.make_async_remote_copy(
        unit, unit_in, unit_send, unit_recv, device_id=across, device_id_type=MESH
    )

    def send_parts():
        unit_copy.start()
        for c in range(N_SUB):
            part_copy(c).start()

    @pl.when(s == 0)
    def _():
        send_parts()

    pair_copy = pltpu.make_async_remote_copy(
        pairs.at[far], pairs.at[far], pair_send, pair_recv,
        device_id={"dp": ((1 - far) * n_near + near) * INNER + y, "section": s, "tensor": x},
        device_id_type=MESH,
    )
    pair_copy.start()

    first(1)
    second(1)

    @pl.when(s == 1)
    def _():
        send_parts()

    unit_copy.wait_recv()
    units[...] = jnp.broadcast_to(to_column(unit_in[...], own_rows), (own_rows, 128))

    def piece(block, c):
        return held.at[block, pl.ds(c * sub, sub)]

    def held_copy(block, c, to, sem):
        return pltpu.make_async_remote_copy(
            piece(block, c), piece(block, c), sem, held_recv.at[c, block],
            device_id=to, device_id_type=MESH,
        )

    def core_copy(block, c):
        return pltpu.make_async_remote_copy(
            piece(block, c), other.at[block, pl.ds(c * sub, sub)], core_send.at[c, block],
            other_recv.at[block], device_id=partner, device_id_type=MESH,
        )

    beside = member(s, 1 - my_a, my_b, s)
    beside_partner = member(s, 1 - my_a, my_b, 1 - s)

    def cross_copy(block, c, sem):
        return pltpu.make_async_remote_copy(
            piece(block, c), other.at[block, pl.ds(c * sub, sub)], sem, other_recv.at[block],
            device_id=beside_partner, device_id_type=MESH,
        )

    def at_b(k):
        return lax.rem(my_b + k, my_n)

    def beyond(k):
        return member(s, my_a, at_b(k), s)

    def arrived(block, c, begin):
        if begin:
            wait_bytes(piece(block, c), held_recv.at[c, block])
            core_copy(block, c).start()
        else:
            core_copy(block, c).wait_send()

    def act_on(kind, c, begin):
        run = lambda copy: copy.start() if begin else copy.wait_send()
        if kind == "P":
            if begin:
                rows = pl.ds(c * sub, sub)
                part_copy(c).wait_recv()
                theirs = from_fixed(fixed_in[rows], units[rows, 0:1])
                raw = (part[rows] + theirs) + xs[
                    pl.ds(own_rows + c * sub, sub)
                ].astype(jnp.float32)
                norms = lax.rsqrt(jnp.sum(raw * raw, axis=-1, keepdims=True) + 1e-06)
                held[mine, rows] = (raw * norms).astype(jnp.bfloat16)
            others(my_n, lambda k: run(held_copy(mine, c, beyond(k), far_send.at[c, k])))
            run(held_copy(mine, c, beside, near_send.at[c]))
            run(core_copy(mine, c))
        elif kind == "A":
            arrived(block_of(1 - my_a, my_b), c, begin)
        elif kind == "B":
            def from_b(k):
                block = block_of(my_a, at_b(k))
                if begin:
                    wait_bytes(piece(block, c), held_recv.at[c, block])
                run(cross_copy(block, c, cross_send.at[c, k]))
                run(held_copy(block, c, beside, fwd_send.at[c, k]))
                run(core_copy(block, c))

            others(my_n, from_b)
        elif begin:
            def from_both(k):
                block = block_of(1 - my_a, at_b(k))
                wait_bytes(piece(block, c), held_recv.at[c, block])

            others(my_n, from_both)

    scale_value, bias_value = scale_ref[...], bias_ref[...]
    width = held.shape[2]
    slot = d * n_tensor + x

    def loss_copy(n):
        return pltpu.make_async_remote_copy(
            loss_row, loss_all.at[slot], loss_send, loss_recv,
            device_id=device_of(n), device_id_type=MESH,
        )

    def send_loss():
        loss_row[...] = jnp.sum(loss_acc[...], axis=0, keepdims=True)
        loss_all[slot] = loss_row[...]

        def body(n, carry):
            loss_copy(lax.rem(me + n, n_all)).start()
            return carry

        lax.fori_loop(1, n_all, body, 0)

    def tile_of(ref, tile):
        return ref[pl.ds(tile * tile_blocks, tile_blocks)].reshape(tile_rows, width)

    def score(tower, a, tile):
        slides, reports = (held, other) if tower == 0 else (other, held)
        logits = scale_value * lax.dot_general(
            slides[pl.ds(a * PAIR, PAIR)].reshape(rows_dp, width), tile_of(reports, tile),
            (((1,), (1,)), ((), ())), preferred_element_type=jnp.float32,
        ) + bias_value
        rows = pl.ds(pl.multiple_of(a * rows_dp, 16), rows_dp)
        shift = tile * (PAIR * INNER * rows_dp)
        for j in range(tile_rows // 128):
            lanes = slice(j * 128, (j + 1) * 128)
            sign = jnp.where(left[rows] == right[:, lanes] + shift, 1.0, -1.0).astype(jnp.float32)
            u = -sign * logits[:, lanes]
            e = jnp.exp(-jnp.abs(u))
            if tower == 1:
                loss_acc[...] += jnp.maximum(u, 0.0) + jnp.log1p(e)
            sigmoid = jnp.where(u >= 0, 1.0, e) / (1.0 + e)
            scores[rows, lanes] = (-scale_value * sign * sigmoid).astype(jnp.bfloat16)

    def slide_terms(a, tile):
        return jnp.dot(
            scores[pl.ds(pl.multiple_of(a * rows_dp, 16), rows_dp)], tile_of(other, tile),
            preferred_element_type=jnp.float32,
        ).reshape(PAIR, own_rows, width)

    def report_terms():
        return lax.dot_general(
            scores[...], tile_of(other, 0), (((0,), (0,)), ((), ())),
            preferred_element_type=jnp.float32,
        ).reshape(tile_blocks, own_rows, width)

    part_rows = own_rows // R_SUB

    def sent_copy(block, c, target, to, sem):
        return pltpu.make_async_remote_copy(
            sent.at[block, pl.ds(c * part_rows, part_rows)], target, sent_send.at[block, c], sem,
            device_id=to, device_id_type=MESH,
        )

    def sent_unit_copy(block, h, target, to, sem):
        return pltpu.make_async_remote_copy(
            sent_unit.at[block, h], target, sent_unit_send.at[block, h], sem,
            device_id=to, device_id_type=MESH,
        )

    def owner_unit_copy(block, h, a, b):
        return sent_unit_copy(
            block, h, got_unit.at[s, my_b], member(s, a, b, h), got_unit_recv.at[s, my_b]
        )

    def owner_copy(block, c, a, b):
        per = R_SUB // n_section
        return sent_copy(
            block, c, got.at[s, my_b, pl.ds(c % per * part_rows, part_rows)], member(s, a, b, c // per),
            got_recv.at[s, my_b],
        )

    def halves_to_rows(block, units_of):
        for h in range(n_section):
            sent_unit[block, h] = to_row(units_of[h * quarter:(h + 1) * quarter])

    def send_across(k, begin):
        b = at_b(k)
        block = block_of(1 - my_a, b)
        copies = [sent_unit_copy(block, 0, relay_unit.at[b], beside, relay_unit_recv.at[b])]
        copies += [
            sent_copy(block, c, relay.at[b, pl.ds(c * part_rows, part_rows)], beside, relay_recv.at[b, c])
            for c in range(R_SUB)
        ]
        if begin:
            values, units_of = to_fixed(grad[block])
            sent[block] = values
            sent_unit[block, 0] = to_row(units_of)
        for copy in copies:
            copy.start() if begin else copy.wait_send()

    def send_beside(begin):
        block = block_of(1 - my_a, my_b)
        if begin:
            values, units_of = to_fixed(grad[block])
            sent[block] = values
            halves_to_rows(block, units_of)
        for h in range(n_section):
            copy = owner_unit_copy(block, h, 1 - my_a, my_b)
            copy.start() if begin else copy.wait_send()
        for c in range(R_SUB):
            copy = owner_copy(block, c, 1 - my_a, my_b)
            copy.start() if begin else copy.wait_send()

    def pass_on(k, begin):
        b = at_b(k)
        block = block_of(my_a, b)
        if begin:
            top = jnp.max(jnp.abs(grad[block]), axis=-1, keepdims=True)
            wait_bytes(relay_unit.at[b], relay_unit_recv.at[b])
            came = to_column(relay_unit[b], own_rows)
            units_of = jnp.maximum(top, 1e-30) * (1.0 / TOP) + came
            halves_to_rows(block, units_of)
            inverse = 1.0 / units_of
        for h in range(n_section):
            copy = owner_unit_copy(block, h, my_a, b)
            copy.start() if begin else copy.wait_send()
        for c in range(R_SUB):
            if begin:
                rows = slice(c * part_rows, (c + 1) * part_rows)
                wait_bytes(relay.at[b, pl.ds(c * part_rows, part_rows)], relay_recv.at[b, c])
                value = grad[block, rows] + from_fixed(relay[b, rows], came[rows])
                sent[block, rows] = jnp.round(value * inverse[rows]).astype(jnp.int32).astype(jnp.int16)
            copy = owner_copy(block, c, my_a, b)
            copy.start() if begin else copy.wait_send()

    twin_copy = pltpu.make_async_remote_copy(
        grad.at[mine, pl.ds(pl.multiple_of((1 - s) * quarter, 16), quarter)], twin,
        twin_send, twin_recv, device_id=partner, device_id_type=MESH,
    )

    def other_block(block):
        wait_bytes(other.at[block], other_recv.at[block])

    def make_ids():
        right[...] = report_ids(iota((1, tile_rows), 1))
        pair_copy.wait_recv()
        for b in range(PAIR):
            column = to_column(pairs[b].astype(jnp.float32), rows_dp).astype(jnp.int32)
            for a in range(n_tensor):
                at = (a * PAIR + b) * own_rows
                left[at:at + own_rows] = jnp.broadcast_to(
                    column[a * own_rows:(a + 1) * own_rows], (own_rows, 128)
                )

    def run_tower(tower):
        for kind, c in events(tower):
            act_on(kind, c, True)
            if (kind, c) == ("P", N_SUB - 1):
                make_ids()
        if n_tiles > 1:
            def wait_block(block, carry):
                other_block(block)
                return carry

            lax.fori_loop(0, 2 * (n_near if tower == 0 else PAIR), wait_block, 0)
            if tower == 0:
                grad[0:tile_blocks] = jnp.zeros_like(grad[0:tile_blocks])

            def tile_step(tile, carry):
                for a in range(2):
                    score(tower, a, tile)
                    if tower == 0:
                        grad[a * PAIR:(a + 1) * PAIR] += slide_terms(a, tile)
                if tower == 1:
                    grad[pl.ds(tile * tile_blocks, tile_blocks)] = report_terms()
                return carry

            lax.fori_loop(0, n_tiles, tile_step, 0)
            others(my_n, lambda k: send_across(k, True))
            send_beside(True)
        elif tower == 0:
            for block in range(tile_blocks):
                other_block(block)
            score(tower, 1 - my_a, 0)
            grad[pl.ds((1 - my_a) * PAIR, PAIR)] = slide_terms(1 - my_a, 0)
            send_across(1, True)
            send_beside(True)
            score(tower, my_a, 0)
            grad[pl.ds(my_a * PAIR, PAIR)] = slide_terms(my_a, 0)
        else:
            for a in (x, 1 - x):
                for b in (far, 1 - far):
                    other_block(block_of(a, b))
                score(tower, a, 0)
            grad[...] = report_terms()
            send_across(1, True)
            send_beside(True)
        if tower == 1:
            send_loss()
        twin_copy.start()
        others(my_n, lambda k: pass_on(k, True))

    for tower in range(n_section):
        @pl.when(s == tower)
        def _():
            run_tower(tower)

    def add_got(t, b, out):
        wait_bytes(got_unit.at[t, b], got_unit_recv.at[t, b])
        wait_bytes(got.at[t, b], got_recv.at[t, b])
        out[...] += from_fixed(got[t, b], to_column(got_unit[t, b], quarter))

    def collect(t, out):
        _, b, count = place_of(t)
        add_got(t, b, out)
        others(count, lambda k: add_got(t, lax.rem(b + k, count), out))

    mine_out[...] = grad[mine, pl.ds(pl.multiple_of(s * quarter, 16), quarter)]
    twin_copy.wait_recv()
    theirs_out[...] = twin[...]
    collect(s, mine_out)
    collect(1 - s, theirs_out)
    for c in range(N_SUB):
        part_copy(c).wait_send()
    unit_copy.wait_send()
    pair_copy.wait_send()
    for kind, c in events(0):
        act_on(kind, c, False)
    others(my_n, lambda k: send_across(k, False))
    send_beside(False)
    others(my_n, lambda k: pass_on(k, False))
    twin_copy.wait_send()
    n_chips = n_dp * n_tensor

    @pl.when(s == 1)
    def _():
        wait_bytes(loss_all.at[pl.ds(0, n_all - 1)], loss_send)
        wait_bytes(loss_all.at[pl.ds(0, n_chips - 1)], loss_recv)

    @pl.when(s != 1)
    def _():
        wait_bytes(loss_all.at[pl.ds(0, n_chips)], loss_recv)

    loss_out[...] = jnp.broadcast_to(jnp.sum(loss_all[0:n_chips]) / total, loss_out.shape)


def local(tower_input, up_weight, down_weight, pair, scale, bias):
    n_dp = lax.axis_size("dp")
    n_section = lax.axis_size("section")
    n_tensor = lax.axis_size("tensor")
    inputs, up_w, down_w = tower_input[0], up_weight[0], down_weight[0]
    rows, width = inputs.shape
    hidden = up_w.shape[1]
    group = n_section * n_tensor
    quarter = rows // group
    own_rows = n_section * quarter
    total = n_dp * rows
    n_near = n_dp // (INNER * PAIR)
    blocks = 2 * n_near
    tile_rows = 2 * PAIR * own_rows

    f32, bf16, i16, i32 = jnp.float32, jnp.bfloat16, jnp.int16, jnp.int32
    vmem = pl.BlockSpec(memory_space=pltpu.VMEM)
    hbm = pl.BlockSpec(memory_space=pl.ANY)
    dma = pltpu.SemaphoreType.DMA
    n_all = n_dp * group
    dims = (n_dp, n_section, n_tensor, n_near, total)
    loss, mine, theirs = pl.pallas_call(
        functools.partial(kernel, dims),
        out_shape=(
            jax.ShapeDtypeStruct((1, 128), f32),
            jax.ShapeDtypeStruct((quarter, width), f32),
            jax.ShapeDtypeStruct((quarter, width), f32),
        ),
        in_specs=[hbm] * 6,
        out_specs=(vmem, vmem, vmem),
        scratch_shapes=[
            pltpu.VMEM((rows, width), bf16),
            pltpu.VMEM((width, hidden), bf16),
            pltpu.VMEM((hidden, width), bf16),
            pltpu.VMEM((rows, hidden), bf16),
            pltpu.VMEM((own_rows, width), f32),
            pltpu.VMEM((own_rows, width), i16),
            pltpu.VMEM((own_rows, width), i16),
            pltpu.VMEM((1, 128), f32),
            pltpu.VMEM((1, 128), f32),
            pltpu.VMEM((own_rows, 128), f32),
            pltpu.VMEM((PAIR, 1, rows), i32),
            pltpu.VMEM((tile_rows, 128), i32),
            pltpu.VMEM((1, tile_rows), i32),
            pltpu.VMEM((blocks, own_rows, width), bf16),
            pltpu.VMEM((blocks, own_rows, width), bf16),
            pltpu.VMEM((tile_rows, tile_rows), bf16),
            pltpu.VMEM((blocks, own_rows, width), f32),
            pltpu.VMEM((blocks, own_rows, width), i16),
            pltpu.VMEM((blocks, n_section, 1, 128), f32),
            pltpu.VMEM((n_near, own_rows, width), i16),
            pltpu.VMEM((n_near, 1, 128), f32),
            pltpu.VMEM((n_section, n_near, quarter, width), i16),
            pltpu.VMEM((n_section, n_near, 1, 128), f32),
            pltpu.VMEM((quarter, width), f32),
            pltpu.VMEM((rows, 128), f32),
            pltpu.VMEM((1, 128), f32),
            pltpu.VMEM((n_all, 1, 128), f32),
            pltpu.VMEM((1, 1), f32),
            pltpu.VMEM((1, 1), f32),
            pltpu.VMEM((1, rows), i32),
            dma((3,)),
            dma((group,)),
            dma((UP_PARTS,)),
            dma((DOWN_PARTS,)),
            dma((N_SUB,)),
            dma((N_SUB,)),
            dma, dma, dma, dma,
            dma((N_SUB, blocks)),
            dma((N_SUB,)),
            dma((N_SUB, n_near)),
            dma((N_SUB, n_near)),
            dma((N_SUB, n_near)),
            dma((N_SUB, blocks)),
            dma((blocks,)),
            dma((blocks, R_SUB)),
            dma((blocks, n_section)),
            dma((n_near, R_SUB)),
            dma((n_near,)),
            dma((n_section, n_near)),
            dma((n_section, n_near)),
            dma, dma, dma, dma,
        ],
        compiler_params=pltpu.CompilerParams(
            collective_id=0, has_side_effects=True, vmem_limit_bytes=52 * 1024 * 1024
        ),
    )(scale.reshape(1, 1), bias.reshape(1, 1), *(
        pltpu.with_memory_space_constraint(a, pltpu.HBM)
        for a in (pair.reshape(1, rows), inputs, up_w, down_w)
    ))
    first_core = lax.axis_index("section") == 0
    return (
        loss[0, :1],
        jnp.where(first_core, mine, theirs),
        jnp.where(first_core, theirs, mine),
    )


def solution(mesh):
    return jax.shard_map(
        local,
        mesh=mesh,
        in_specs=(
            P("section", "dp", None),
            P("section", None, "tensor"),
            P("section", "tensor", None),
            P("dp"),
            P(),
            P(),
        ),
        out_specs=(P(), P(("dp", "section", "tensor"), None), P(("dp", "section", "tensor"), None)),
        check_vma=False,
    )
```

```python
import functools

import jax
import jax.numpy as jnp
from jax import lax
from jax.experimental import pallas as pl
from jax.experimental.pallas import tpu as pltpu
from jax.sharding import PartitionSpec as P

MESH = pl.DeviceIdType.MESH
INNER = 2
PAIR = 2
UP_PARTS = 2
DOWN_PARTS = 1
N_SUB = 6
DIRECT = 3
R_SUB = 6
TOP = 32767.0


TIMES = (
    {"A": (4.0, 0.40), "B": (3.2, 0.70), "D": (5.4, 0.70)},
    {"A": (2.6, 0.50), "B": (2.7, 0.55), "D": (5.0, 0.55)},
)


def events(tower):
    found = [
        (start + c * step, "ABD".index(kind), kind, c)
        for kind, (start, step) in TIMES[tower].items() for c in range(N_SUB)
    ]
    return [("P", c) for c in range(N_SUB)] + [(kind, c) for _, _, kind, c in sorted(found)]


def wait_bytes(ref, sem):
    pltpu.make_async_copy(ref, ref, sem).wait()


def iota(shape, dim):
    return lax.broadcasted_iota(jnp.int32, shape, dim)


def step_of(value, size, count):
    return sum((value >= i * size).astype(jnp.int32) for i in range(1, count))


def to_row(column, lanes=128):
    rows = column.shape[0]
    hit = iota((rows, lanes), 0) == iota((rows, lanes), 1)
    return jnp.sum(jnp.where(hit, column, 0.0), axis=0, keepdims=True)


def to_column(row, rows):
    hit = iota((rows, row.shape[1]), 0) == iota((rows, row.shape[1]), 1)
    return jnp.sum(jnp.where(hit, row, 0.0), axis=1, keepdims=True)


def to_fixed(value):
    top = jnp.maximum(jnp.max(jnp.abs(value), axis=-1, keepdims=True), 1e-30)
    fixed = jnp.round(value * (TOP / top)).astype(jnp.int32).astype(jnp.int16)
    return fixed, top * (1.0 / TOP)


def from_fixed(fixed, unit):
    return fixed.astype(jnp.int32).astype(jnp.float32) * unit


def kernel(
    dims,
    scale_in, bias_in, pair_in, x_ref, up_ref, down_ref,
    loss_out, mine_out, theirs_out,
    xs, up, down, hid, part, fixed, fixed_in, unit, unit_in, units, pairs, left, right,
    held, other, scores, grad, sent, sent_unit, relay, relay_unit, got, got_unit, twin,
    loss_acc, loss_row, loss_all, scale_ref, bias_ref, pair_ref,
    small_sem, x_sem, up_sem, down_sem, part_send, part_recv, unit_send, unit_recv, pair_send, pair_recv,
    held_recv, near_send, far_send, fwd_send, cross_send, core_send, other_recv,
    sent_send, sent_unit_send, relay_recv, relay_unit_recv, got_recv, got_unit_recv,
    twin_send, twin_recv, loss_send, loss_recv,
):
    n_dp, n_section, n_tensor, n_near, total = dims
    quarter = xs.shape[0] // (n_section * n_tensor)
    own_rows = n_section * quarter
    rows_dp = xs.shape[0]
    d, s, x = lax.axis_index("dp"), lax.axis_index("section"), lax.axis_index("tensor")
    y, near, far = lax.rem(d, INNER), lax.rem(d // INNER, n_near), d // (INNER * n_near)
    n_all = n_dp * n_section * n_tensor
    me = (d * n_section + s) * n_tensor + x
    tile_blocks = 2 * PAIR
    tile_rows = tile_blocks * own_rows
    n_tiles = n_near // PAIR

    def device_of(n):
        return {
            "dp": n // (n_section * n_tensor),
            "section": lax.rem(n // n_tensor, n_section),
            "tensor": lax.rem(n, n_tensor),
        }

    def pick(t, first, second):
        return first + t * (second - first)

    def member(t, a, b, core):
        at_y, at_near, at_far = pick(t, y, a), pick(t, near, b), pick(t, b, far)
        return {
            "dp": (at_far * n_near + at_near) * INNER + at_y, "section": core,
            "tensor": pick(t, a, x),
        }

    def place_of(t):
        return pick(t, x, y), pick(t, far, near), pick(t, PAIR, n_near)

    my_a, my_b, my_n = place_of(s)
    def block_of(a, b):
        return (b // PAIR) * tile_blocks + a * PAIR + lax.rem(b, PAIR)

    mine = block_of(my_a, my_b)
    partner = {"dp": d, "section": 1 - s, "tensor": x}

    def others(count, act):
        if n_near == PAIR:
            act(1)
        else:
            def body(k, carry):
                act(k)
                return carry
            lax.fori_loop(1, count, body, 0)

    x_copies = []
    for side, t in ((0, 1 - x), (1, x)):
        for q in range(n_section):
            x_copies.append(pltpu.make_async_copy(
                x_ref.at[pl.ds(pl.multiple_of((q * n_tensor + t) * quarter, 16), quarter)],
                xs.at[pl.ds(side * own_rows + q * quarter, quarter)],
                x_sem.at[side * n_section + q],
            ))
    small_copies = [
        pltpu.make_async_copy(here, there, small_sem.at[i])
        for i, (here, there) in enumerate(
            ((pair_in, pair_ref), (scale_in, scale_ref), (bias_in, bias_ref))
        )
    ]
    for c in small_copies:
        c.start()
    for c in x_copies:
        c.start()
    up_w = up.shape[1] // UP_PARTS
    down_w = down.shape[1] // DOWN_PARTS

    def up_copy(i):
        cols = pl.ds(i * up_w, up_w)
        return pltpu.make_async_copy(up_ref.at[:, cols], up.at[:, cols], up_sem.at[i])

    def down_copy(i):
        cols = pl.ds(i * down_w, down_w)
        return pltpu.make_async_copy(down_ref.at[:, cols], down.at[:, cols], down_sem.at[i])

    for i in range(UP_PARTS):
        up_copy(i).start()
    for i in range(DOWN_PARTS):
        down_copy(i).start()

    barrier = pltpu.get_barrier_semaphore()

    def greet(n, carry):
        @pl.when(n != me)
        def _():
            pl.semaphore_signal(barrier, inc=1, device_id=device_of(n), device_id_type=MESH)
        return carry

    lax.fori_loop(0, n_all, greet, 0)
    loss_acc[...] = jnp.zeros_like(loss_acc)

    def natural(lane, t):
        q = step_of(lane, quarter, n_section)
        return (q * n_tensor + t) * quarter + (lane - q * quarter)

    def order_pairs():
        column = to_column(pair_ref[...].astype(jnp.float32), rows_dp)
        lane = iota((rows_dp, rows_dp), 1)
        t = step_of(lane, own_rows, n_tensor)
        hit = iota((rows_dp, rows_dp), 0) == natural(lane - t * own_rows, t)
        pairs[far] = jnp.sum(jnp.where(hit, column, 0.0), axis=0, keepdims=True).astype(jnp.int32)

    for c in small_copies:
        c.wait()
    order_pairs()

    def report_ids(index):
        block = step_of(index, own_rows, tile_blocks)
        a = step_of(block, PAIR, 2)
        home = (far * n_near + block - PAIR * a) * INNER + a
        return home * rows_dp + natural(index - block * own_rows, x)

    for c in x_copies:
        c.wait()

    def first(side):
        rows = pl.ds(side * own_rows, own_rows)

        def body(i, carry):
            if side == 0:
                up_copy(i).wait()
            cols = pl.ds(i * up_w, up_w)
            h = jnp.dot(xs[rows], up[:, cols], preferred_element_type=jnp.float32)
            hid[rows, cols] = jax.nn.gelu(h).astype(jnp.bfloat16)
            return carry

        for i in range(UP_PARTS):
            body(i, 0)

    def second(side):
        def body(i, carry):
            if side == 0:
                down_copy(i).wait()
            cols = pl.ds(i * down_w, down_w)
            part[:, cols] = jnp.dot(
                hid[side * own_rows:(side + 1) * own_rows], down[:, cols],
                preferred_element_type=jnp.float32,
            )
            return carry

        for i in range(DOWN_PARTS):
            body(i, 0)

    first(0)
    second(0)
    values, units_of = to_fixed(part[...])
    fixed[...] = values
    unit[...] = to_row(units_of)
    pl.semaphore_wait(barrier, n_all - 1)

    sub = own_rows // N_SUB
    across = {"dp": d, "section": s, "tensor": 1 - x}

    def part_copy(c):
        rows = pl.ds(c * sub, sub)
        return pltpu.make_async_remote_copy(
            fixed.at[rows], fixed_in.at[rows], part_send.at[c], part_recv.at[c],
            device_id=across, device_id_type=MESH,
        )

    unit_copy = pltpu.make_async_remote_copy(
        unit, unit_in, unit_send, unit_recv, device_id=across, device_id_type=MESH
    )

    def send_parts():
        unit_copy.start()
        for c in range(N_SUB):
            part_copy(c).start()

    @pl.when(s == 0)
    def _():
        send_parts()

    pair_copy = pltpu.make_async_remote_copy(
        pairs.at[far], pairs.at[far], pair_send, pair_recv,
        device_id={"dp": ((1 - far) * n_near + near) * INNER + y, "section": s, "tensor": x},
        device_id_type=MESH,
    )
    pair_copy.start()

    first(1)
    second(1)

    @pl.when(s == 1)
    def _():
        send_parts()

    unit_copy.wait_recv()
    units[...] = jnp.broadcast_to(to_column(unit_in[...], own_rows), (own_rows, 128))

    def piece(block, c):
        return held.at[block, pl.ds(c * sub, sub)]

    def held_copy(block, c, to, sem):
        return pltpu.make_async_remote_copy(
            piece(block, c), piece(block, c), sem, held_recv.at[c, block],
            device_id=to, device_id_type=MESH,
        )

    def core_copy(block, c):
        return pltpu.make_async_remote_copy(
            piece(block, c), other.at[block, pl.ds(c * sub, sub)], core_send.at[c, block],
            other_recv.at[block], device_id=partner, device_id_type=MESH,
        )

    beside = member(s, 1 - my_a, my_b, s)
    beside_partner = member(s, 1 - my_a, my_b, 1 - s)

    def cross_copy(block, c, sem):
        return pltpu.make_async_remote_copy(
            piece(block, c), other.at[block, pl.ds(c * sub, sub)], sem, other_recv.at[block],
            device_id=beside_partner, device_id_type=MESH,
        )

    def at_b(k):
        return lax.rem(my_b + k, my_n)

    def beyond(k):
        return member(s, my_a, at_b(k), s)

    def arrived(block, c, begin):
        if begin:
            wait_bytes(piece(block, c), held_recv.at[c, block])
            core_copy(block, c).start()
        else:
            core_copy(block, c).wait_send()

    def act_on(kind, c, begin):
        run = lambda copy: copy.start() if begin else copy.wait_send()
        if kind == "P":
            if begin:
                rows = pl.ds(c * sub, sub)
                part_copy(c).wait_recv()
                theirs = from_fixed(fixed_in[rows], units[rows, 0:1])
                raw = (part[rows] + theirs) + xs[
                    pl.ds(own_rows + c * sub, sub)
                ].astype(jnp.float32)
                norms = lax.rsqrt(jnp.sum(raw * raw, axis=-1, keepdims=True) + 1e-06)
                held[mine, rows] = (raw * norms).astype(jnp.bfloat16)
            others(my_n, lambda k: run(held_copy(mine, c, beyond(k), far_send.at[c, k])))
            run(held_copy(mine, c, beside, near_send.at[c]))
            run(core_copy(mine, c))
        elif kind == "A":
            arrived(block_of(1 - my_a, my_b), c, begin)
        elif kind == "B":
            def from_b(k):
                block = block_of(my_a, at_b(k))
                if begin:
                    wait_bytes(piece(block, c), held_recv.at[c, block])
                if c >= DIRECT:
                    run(cross_copy(block, c, cross_send.at[c, k]))
                run(held_copy(block, c, beside, fwd_send.at[c, k]))
                run(core_copy(block, c))

            others(my_n, from_b)
        else:
            def from_both(k):
                block = block_of(1 - my_a, at_b(k))
                if begin:
                    wait_bytes(piece(block, c), held_recv.at[c, block])
                if c < DIRECT:
                    run(core_copy(block, c))

            others(my_n, from_both)

    scale_value, bias_value = scale_ref[...], bias_ref[...]
    width = held.shape[2]
    slot = d * n_tensor + x

    def loss_copy(n):
        return pltpu.make_async_remote_copy(
            loss_row, loss_all.at[slot], loss_send, loss_recv,
            device_id=device_of(n), device_id_type=MESH,
        )

    def send_loss():
        loss_row[...] = jnp.sum(loss_acc[...], axis=0, keepdims=True)
        loss_all[slot] = loss_row[...]

        def body(n, carry):
            loss_copy(lax.rem(me + n, n_all)).start()
            return carry

        lax.fori_loop(1, n_all, body, 0)

    def tile_of(ref, tile):
        return ref[pl.ds(tile * tile_blocks, tile_blocks)].reshape(tile_rows, width)

    def score(tower, a, tile):
        slides, reports = (held, other) if tower == 0 else (other, held)
        logits = scale_value * lax.dot_general(
            slides[pl.ds(a * PAIR, PAIR)].reshape(rows_dp, width), tile_of(reports, tile),
            (((1,), (1,)), ((), ())), preferred_element_type=jnp.float32,
        ) + bias_value
        rows = pl.ds(pl.multiple_of(a * rows_dp, 16), rows_dp)
        shift = tile * (PAIR * INNER * rows_dp)
        for j in range(tile_rows // 128):
            lanes = slice(j * 128, (j + 1) * 128)
            sign = jnp.where(left[rows] == right[:, lanes] + shift, 1.0, -1.0).astype(jnp.float32)
            u = -sign * logits[:, lanes]
            e = jnp.exp(-jnp.abs(u))
            if tower == 1:
                loss_acc[...] += jnp.maximum(u, 0.0) + jnp.log1p(e)
            sigmoid = jnp.where(u >= 0, 1.0, e) / (1.0 + e)
            scores[rows, lanes] = (-scale_value * sign * sigmoid).astype(jnp.bfloat16)

    def slide_terms(a, tile):
        return jnp.dot(
            scores[pl.ds(pl.multiple_of(a * rows_dp, 16), rows_dp)], tile_of(other, tile),
            preferred_element_type=jnp.float32,
        ).reshape(PAIR, own_rows, width)

    def report_terms():
        return lax.dot_general(
            scores[...], tile_of(other, 0), (((0,), (0,)), ((), ())),
            preferred_element_type=jnp.float32,
        ).reshape(tile_blocks, own_rows, width)

    part_rows = own_rows // R_SUB

    def sent_copy(block, c, target, to, sem):
        return pltpu.make_async_remote_copy(
            sent.at[block, pl.ds(c * part_rows, part_rows)], target, sent_send.at[block, c], sem,
            device_id=to, device_id_type=MESH,
        )

    def sent_unit_copy(block, h, target, to, sem):
        return pltpu.make_async_remote_copy(
            sent_unit.at[block, h], target, sent_unit_send.at[block, h], sem,
            device_id=to, device_id_type=MESH,
        )

    def owner_unit_copy(block, h, a, b):
        return sent_unit_copy(
            block, h, got_unit.at[s, my_b], member(s, a, b, h), got_unit_recv.at[s, my_b]
        )

    def owner_copy(block, c, a, b):
        per = R_SUB // n_section
        return sent_copy(
            block, c, got.at[s, my_b, pl.ds(c % per * part_rows, part_rows)], member(s, a, b, c // per),
            got_recv.at[s, my_b],
        )

    def halves_to_rows(block, units_of):
        for h in range(n_section):
            sent_unit[block, h] = to_row(units_of[h * quarter:(h + 1) * quarter])

    def send_across(k, begin):
        b = at_b(k)
        block = block_of(1 - my_a, b)
        copies = [sent_unit_copy(block, 0, relay_unit.at[b], beside, relay_unit_recv.at[b])]
        copies += [
            sent_copy(block, c, relay.at[b, pl.ds(c * part_rows, part_rows)], beside, relay_recv.at[b, c])
            for c in range(R_SUB)
        ]
        if begin:
            values, units_of = to_fixed(grad[block])
            sent[block] = values
            sent_unit[block, 0] = to_row(units_of)
        for copy in copies:
            copy.start() if begin else copy.wait_send()

    def send_beside(begin):
        block = block_of(1 - my_a, my_b)
        if begin:
            values, units_of = to_fixed(grad[block])
            sent[block] = values
            halves_to_rows(block, units_of)
        for h in range(n_section):
            copy = owner_unit_copy(block, h, 1 - my_a, my_b)
            copy.start() if begin else copy.wait_send()
        for c in range(R_SUB):
            copy = owner_copy(block, c, 1 - my_a, my_b)
            copy.start() if begin else copy.wait_send()

    def pass_on(k, begin):
        b = at_b(k)
        block = block_of(my_a, b)
        if begin:
            top = jnp.max(jnp.abs(grad[block]), axis=-1, keepdims=True)
            wait_bytes(relay_unit.at[b], relay_unit_recv.at[b])
            came = to_column(relay_unit[b], own_rows)
            units_of = jnp.maximum(top, 1e-30) * (1.0 / TOP) + came
            halves_to_rows(block, units_of)
            inverse = 1.0 / units_of
        for h in range(n_section):
            copy = owner_unit_copy(block, h, my_a, b)
            copy.start() if begin else copy.wait_send()
        for c in range(R_SUB):
            if begin:
                rows = slice(c * part_rows, (c + 1) * part_rows)
                wait_bytes(relay.at[b, pl.ds(c * part_rows, part_rows)], relay_recv.at[b, c])
                value = grad[block, rows] + from_fixed(relay[b, rows], came[rows])
                sent[block, rows] = jnp.round(value * inverse[rows]).astype(jnp.int32).astype(jnp.int16)
            copy = owner_copy(block, c, my_a, b)
            copy.start() if begin else copy.wait_send()

    twin_copy = pltpu.make_async_remote_copy(
        grad.at[mine, pl.ds(pl.multiple_of((1 - s) * quarter, 16), quarter)], twin,
        twin_send, twin_recv, device_id=partner, device_id_type=MESH,
    )

    def other_block(block):
        wait_bytes(other.at[block], other_recv.at[block])

    def make_ids():
        right[...] = report_ids(iota((1, tile_rows), 1))
        pair_copy.wait_recv()
        for b in range(PAIR):
            column = to_column(pairs[b].astype(jnp.float32), rows_dp).astype(jnp.int32)
            for a in range(n_tensor):
                at = (a * PAIR + b) * own_rows
                left[at:at + own_rows] = jnp.broadcast_to(
                    column[a * own_rows:(a + 1) * own_rows], (own_rows, 128)
                )

    def run_tower(tower):
        for kind, c in events(tower):
            act_on(kind, c, True)
            if (kind, c) == ("P", N_SUB - 1):
                make_ids()
        if n_tiles > 1:
            def wait_block(block, carry):
                other_block(block)
                return carry

            lax.fori_loop(0, 2 * (n_near if tower == 0 else PAIR), wait_block, 0)
            if tower == 0:
                grad[0:tile_blocks] = jnp.zeros_like(grad[0:tile_blocks])

            def tile_step(tile, carry):
                for a in range(2):
                    score(tower, a, tile)
                    if tower == 0:
                        grad[a * PAIR:(a + 1) * PAIR] += slide_terms(a, tile)
                if tower == 1:
                    grad[pl.ds(tile * tile_blocks, tile_blocks)] = report_terms()
                return carry

            lax.fori_loop(0, n_tiles, tile_step, 0)
            others(my_n, lambda k: send_across(k, True))
            send_beside(True)
        elif tower == 0:
            for block in range(tile_blocks):
                other_block(block)
            score(tower, 1 - my_a, 0)
            grad[pl.ds((1 - my_a) * PAIR, PAIR)] = slide_terms(1 - my_a, 0)
            send_across(1, True)
            send_beside(True)
            score(tower, my_a, 0)
            grad[pl.ds(my_a * PAIR, PAIR)] = slide_terms(my_a, 0)
        else:
            for a in (x, 1 - x):
                for b in (far, 1 - far):
                    other_block(block_of(a, b))
                score(tower, a, 0)
            grad[...] = report_terms()
            send_across(1, True)
            send_beside(True)
        if tower == 1:
            send_loss()
        twin_copy.start()
        others(my_n, lambda k: pass_on(k, True))

    for tower in range(n_section):
        @pl.when(s == tower)
        def _():
            run_tower(tower)

    def add_got(t, b, out):
        wait_bytes(got_unit.at[t, b], got_unit_recv.at[t, b])
        wait_bytes(got.at[t, b], got_recv.at[t, b])
        out[...] += from_fixed(got[t, b], to_column(got_unit[t, b], quarter))

    def collect(t, out):
        _, b, count = place_of(t)
        add_got(t, b, out)
        others(count, lambda k: add_got(t, lax.rem(b + k, count), out))

    mine_out[...] = grad[mine, pl.ds(pl.multiple_of(s * quarter, 16), quarter)]
    twin_copy.wait_recv()
    theirs_out[...] = twin[...]
    collect(s, mine_out)
    collect(1 - s, theirs_out)
    for c in range(N_SUB):
        part_copy(c).wait_send()
    unit_copy.wait_send()
    pair_copy.wait_send()
    for kind, c in events(0):
        act_on(kind, c, False)
    others(my_n, lambda k: send_across(k, False))
    send_beside(False)
    others(my_n, lambda k: pass_on(k, False))
    twin_copy.wait_send()
    n_chips = n_dp * n_tensor

    @pl.when(s == 1)
    def _():
        wait_bytes(loss_all.at[pl.ds(0, n_all - 1)], loss_send)
        wait_bytes(loss_all.at[pl.ds(0, n_chips - 1)], loss_recv)

    @pl.when(s != 1)
    def _():
        wait_bytes(loss_all.at[pl.ds(0, n_chips)], loss_recv)

    loss_out[...] = jnp.broadcast_to(jnp.sum(loss_all[0:n_chips]) / total, loss_out.shape)


def local(tower_input, up_weight, down_weight, pair, scale, bias):
    n_dp = lax.axis_size("dp")
    n_section = lax.axis_size("section")
    n_tensor = lax.axis_size("tensor")
    inputs, up_w, down_w = tower_input[0], up_weight[0], down_weight[0]
    rows, width = inputs.shape
    hidden = up_w.shape[1]
    group = n_section * n_tensor
    quarter = rows // group
    own_rows = n_section * quarter
    total = n_dp * rows
    n_near = n_dp // (INNER * PAIR)
    blocks = 2 * n_near
    tile_rows = 2 * PAIR * own_rows

    f32, bf16, i16, i32 = jnp.float32, jnp.bfloat16, jnp.int16, jnp.int32
    vmem = pl.BlockSpec(memory_space=pltpu.VMEM)
    hbm = pl.BlockSpec(memory_space=pl.ANY)
    dma = pltpu.SemaphoreType.DMA
    n_all = n_dp * group
    dims = (n_dp, n_section, n_tensor, n_near, total)
    loss, mine, theirs = pl.pallas_call(
        functools.partial(kernel, dims),
        out_shape=(
            jax.ShapeDtypeStruct((1, 128), f32),
            jax.ShapeDtypeStruct((quarter, width), f32),
            jax.ShapeDtypeStruct((quarter, width), f32),
        ),
        in_specs=[hbm] * 6,
        out_specs=(vmem, vmem, vmem),
        scratch_shapes=[
            pltpu.VMEM((rows, width), bf16),
            pltpu.VMEM((width, hidden), bf16),
            pltpu.VMEM((hidden, width), bf16),
            pltpu.VMEM((rows, hidden), bf16),
            pltpu.VMEM((own_rows, width), f32),
            pltpu.VMEM((own_rows, width), i16),
            pltpu.VMEM((own_rows, width), i16),
            pltpu.VMEM((1, 128), f32),
            pltpu.VMEM((1, 128), f32),
            pltpu.VMEM((own_rows, 128), f32),
            pltpu.VMEM((PAIR, 1, rows), i32),
            pltpu.VMEM((tile_rows, 128), i32),
            pltpu.VMEM((1, tile_rows), i32),
            pltpu.VMEM((blocks, own_rows, width), bf16),
            pltpu.VMEM((blocks, own_rows, width), bf16),
            pltpu.VMEM((tile_rows, tile_rows), bf16),
            pltpu.VMEM((blocks, own_rows, width), f32),
            pltpu.VMEM((blocks, own_rows, width), i16),
            pltpu.VMEM((blocks, n_section, 1, 128), f32),
            pltpu.VMEM((n_near, own_rows, width), i16),
            pltpu.VMEM((n_near, 1, 128), f32),
            pltpu.VMEM((n_section, n_near, quarter, width), i16),
            pltpu.VMEM((n_section, n_near, 1, 128), f32),
            pltpu.VMEM((quarter, width), f32),
            pltpu.VMEM((rows, 128), f32),
            pltpu.VMEM((1, 128), f32),
            pltpu.VMEM((n_all, 1, 128), f32),
            pltpu.VMEM((1, 1), f32),
            pltpu.VMEM((1, 1), f32),
            pltpu.VMEM((1, rows), i32),
            dma((3,)),
            dma((group,)),
            dma((UP_PARTS,)),
            dma((DOWN_PARTS,)),
            dma((N_SUB,)),
            dma((N_SUB,)),
            dma, dma, dma, dma,
            dma((N_SUB, blocks)),
            dma((N_SUB,)),
            dma((N_SUB, n_near)),
            dma((N_SUB, n_near)),
            dma((N_SUB, n_near)),
            dma((N_SUB, blocks)),
            dma((blocks,)),
            dma((blocks, R_SUB)),
            dma((blocks, n_section)),
            dma((n_near, R_SUB)),
            dma((n_near,)),
            dma((n_section, n_near)),
            dma((n_section, n_near)),
            dma, dma, dma, dma,
        ],
        compiler_params=pltpu.CompilerParams(
            collective_id=0, has_side_effects=True, vmem_limit_bytes=52 * 1024 * 1024
        ),
    )(scale.reshape(1, 1), bias.reshape(1, 1), *(
        pltpu.with_memory_space_constraint(a, pltpu.HBM)
        for a in (pair.reshape(1, rows), inputs, up_w, down_w)
    ))
    first_core = lax.axis_index("section") == 0
    return (
        loss[0, :1],
        jnp.where(first_core, mine, theirs),
        jnp.where(first_core, theirs, mine),
    )


def solution(mesh):
    return jax.shard_map(
        local,
        mesh=mesh,
        in_specs=(
            P("section", "dp", None),
            P("section", None, "tensor"),
            P("section", "tensor", None),
            P("dp"),
            P(),
            P(),
        ),
        out_specs=(P(), P(("dp", "section", "tensor"), None), P(("dp", "section", "tensor"), None)),
        check_vma=False,
    )
```

```python
import functools

import jax
import jax.numpy as jnp
from jax import lax
from jax.experimental import pallas as pl
from jax.experimental.pallas import tpu as pltpu
from jax.sharding import PartitionSpec as P

MESH = pl.DeviceIdType.MESH
INNER = 2
PAIR = 2
UP_PARTS = 2
DOWN_PARTS = 1
N_SUB = 6
DIRECT = 2
R_SUB = 6
TOP = 32767.0


TIMES = (
    {"A": (4.0, 0.40), "B": (3.2, 0.70), "D": (5.4, 0.70)},
    {"A": (2.6, 0.50), "B": (2.7, 0.55), "D": (5.0, 0.55)},
)


def events(tower):
    found = [
        (start + c * step, "ABD".index(kind), kind, c)
        for kind, (start, step) in TIMES[tower].items() for c in range(N_SUB)
    ]
    return [("P", c) for c in range(N_SUB)] + [(kind, c) for _, _, kind, c in sorted(found)]


def wait_bytes(ref, sem):
    pltpu.make_async_copy(ref, ref, sem).wait()


def iota(shape, dim):
    return lax.broadcasted_iota(jnp.int32, shape, dim)


def step_of(value, size, count):
    return sum((value >= i * size).astype(jnp.int32) for i in range(1, count))


def to_row(column, lanes=128):
    rows = column.shape[0]
    hit = iota((rows, lanes), 0) == iota((rows, lanes), 1)
    return jnp.sum(jnp.where(hit, column, 0.0), axis=0, keepdims=True)


def to_column(row, rows):
    hit = iota((rows, row.shape[1]), 0) == iota((rows, row.shape[1]), 1)
    return jnp.sum(jnp.where(hit, row, 0.0), axis=1, keepdims=True)


def to_fixed(value):
    top = jnp.maximum(jnp.max(jnp.abs(value), axis=-1, keepdims=True), 1e-30)
    fixed = jnp.round(value * (TOP / top)).astype(jnp.int32).astype(jnp.int16)
    return fixed, top * (1.0 / TOP)


def from_fixed(fixed, unit):
    return fixed.astype(jnp.int32).astype(jnp.float32) * unit


def kernel(
    dims,
    scale_in, bias_in, pair_in, x_ref, up_ref, down_ref,
    loss_out, mine_out, theirs_out,
    xs, up, down, hid, part, fixed, fixed_in, unit, unit_in, units, pairs, left, right,
    held, other, scores, grad, sent, sent_unit, relay, relay_unit, got, got_unit, twin,
    loss_acc, loss_row, loss_all, scale_ref, bias_ref, pair_ref,
    small_sem, x_sem, up_sem, down_sem, part_send, part_recv, unit_send, unit_recv, pair_send, pair_recv,
    held_recv, near_send, far_send, fwd_send, cross_send, core_send, other_recv,
    sent_send, sent_unit_send, relay_recv, relay_unit_recv, got_recv, got_unit_recv,
    twin_send, twin_recv, loss_send, loss_recv,
):
    n_dp, n_section, n_tensor, n_near, total = dims
    quarter = xs.shape[0] // (n_section * n_tensor)
    own_rows = n_section * quarter
    rows_dp = xs.shape[0]
    d, s, x = lax.axis_index("dp"), lax.axis_index("section"), lax.axis_index("tensor")
    y, near, far = lax.rem(d, INNER), lax.rem(d // INNER, n_near), d // (INNER * n_near)
    n_all = n_dp * n_section * n_tensor
    me = (d * n_section + s) * n_tensor + x
    tile_blocks = 2 * PAIR
    tile_rows = tile_blocks * own_rows
    n_tiles = n_near // PAIR

    def device_of(n):
        return {
            "dp": n // (n_section * n_tensor),
            "section": lax.rem(n // n_tensor, n_section),
            "tensor": lax.rem(n, n_tensor),
        }

    def pick(t, first, second):
        return first + t * (second - first)

    def member(t, a, b, core):
        at_y, at_near, at_far = pick(t, y, a), pick(t, near, b), pick(t, b, far)
        return {
            "dp": (at_far * n_near + at_near) * INNER + at_y, "section": core,
            "tensor": pick(t, a, x),
        }

    def place_of(t):
        return pick(t, x, y), pick(t, far, near), pick(t, PAIR, n_near)

    my_a, my_b, my_n = place_of(s)
    def block_of(a, b):
        return (b // PAIR) * tile_blocks + a * PAIR + lax.rem(b, PAIR)

    mine = block_of(my_a, my_b)
    partner = {"dp": d, "section": 1 - s, "tensor": x}

    def others(count, act):
        if n_near == PAIR:
            act(1)
        else:
            def body(k, carry):
                act(k)
                return carry
            lax.fori_loop(1, count, body, 0)

    x_copies = []
    for side, t in ((0, 1 - x), (1, x)):
        for q in range(n_section):
            x_copies.append(pltpu.make_async_copy(
                x_ref.at[pl.ds(pl.multiple_of((q * n_tensor + t) * quarter, 16), quarter)],
                xs.at[pl.ds(side * own_rows + q * quarter, quarter)],
                x_sem.at[side * n_section + q],
            ))
    small_copies = [
        pltpu.make_async_copy(here, there, small_sem.at[i])
        for i, (here, there) in enumerate(
            ((pair_in, pair_ref), (scale_in, scale_ref), (bias_in, bias_ref))
        )
    ]
    for c in small_copies:
        c.start()
    for c in x_copies:
        c.start()
    up_w = up.shape[1] // UP_PARTS
    down_w = down.shape[1] // DOWN_PARTS

    def up_copy(i):
        cols = pl.ds(i * up_w, up_w)
        return pltpu.make_async_copy(up_ref.at[:, cols], up.at[:, cols], up_sem.at[i])

    def down_copy(i):
        cols = pl.ds(i * down_w, down_w)
        return pltpu.make_async_copy(down_ref.at[:, cols], down.at[:, cols], down_sem.at[i])

    for i in range(UP_PARTS):
        up_copy(i).start()
    for i in range(DOWN_PARTS):
        down_copy(i).start()

    barrier = pltpu.get_barrier_semaphore()

    def greet(n, carry):
        @pl.when(n != me)
        def _():
            pl.semaphore_signal(barrier, inc=1, device_id=device_of(n), device_id_type=MESH)
        return carry

    lax.fori_loop(0, n_all, greet, 0)
    loss_acc[...] = jnp.zeros_like(loss_acc)

    def natural(lane, t):
        q = step_of(lane, quarter, n_section)
        return (q * n_tensor + t) * quarter + (lane - q * quarter)

    def order_pairs():
        column = to_column(pair_ref[...].astype(jnp.float32), rows_dp)
        lane = iota((rows_dp, rows_dp), 1)
        t = step_of(lane, own_rows, n_tensor)
        hit = iota((rows_dp, rows_dp), 0) == natural(lane - t * own_rows, t)
        pairs[far] = jnp.sum(jnp.where(hit, column, 0.0), axis=0, keepdims=True).astype(jnp.int32)

    for c in small_copies:
        c.wait()
    order_pairs()

    def report_ids(index):
        block = step_of(index, own_rows, tile_blocks)
        a = step_of(block, PAIR, 2)
        home = (far * n_near + block - PAIR * a) * INNER + a
        return home * rows_dp + natural(index - block * own_rows, x)

    for c in x_copies:
        c.wait()

    def first(side):
        rows = pl.ds(side * own_rows, own_rows)

        def body(i, carry):
            if side == 0:
                up_copy(i).wait()
            cols = pl.ds(i * up_w, up_w)
            h = jnp.dot(xs[rows], up[:, cols], preferred_element_type=jnp.float32)
            hid[rows, cols] = jax.nn.gelu(h).astype(jnp.bfloat16)
            return carry

        for i in range(UP_PARTS):
            body(i, 0)

    def second(side):
        def body(i, carry):
            if side == 0:
                down_copy(i).wait()
            cols = pl.ds(i * down_w, down_w)
            part[:, cols] = jnp.dot(
                hid[side * own_rows:(side + 1) * own_rows], down[:, cols],
                preferred_element_type=jnp.float32,
            )
            return carry

        for i in range(DOWN_PARTS):
            body(i, 0)

    first(0)
    second(0)
    values, units_of = to_fixed(part[...])
    fixed[...] = values
    unit[...] = to_row(units_of)
    pl.semaphore_wait(barrier, n_all - 1)

    sub = own_rows // N_SUB
    across = {"dp": d, "section": s, "tensor": 1 - x}

    def part_copy(c):
        rows = pl.ds(c * sub, sub)
        return pltpu.make_async_remote_copy(
            fixed.at[rows], fixed_in.at[rows], part_send.at[c], part_recv.at[c],
            device_id=across, device_id_type=MESH,
        )

    unit_copy = pltpu.make_async_remote_copy(
        unit, unit_in, unit_send, unit_recv, device_id=across, device_id_type=MESH
    )

    def send_parts():
        unit_copy.start()
        for c in range(N_SUB):
            part_copy(c).start()

    @pl.when(s == 0)
    def _():
        send_parts()

    pair_copy = pltpu.make_async_remote_copy(
        pairs.at[far], pairs.at[far], pair_send, pair_recv,
        device_id={"dp": ((1 - far) * n_near + near) * INNER + y, "section": s, "tensor": x},
        device_id_type=MESH,
    )
    pair_copy.start()

    first(1)
    second(1)

    @pl.when(s == 1)
    def _():
        send_parts()

    unit_copy.wait_recv()
    units[...] = jnp.broadcast_to(to_column(unit_in[...], own_rows), (own_rows, 128))

    def piece(block, c):
        return held.at[block, pl.ds(c * sub, sub)]

    def held_copy(block, c, to, sem):
        return pltpu.make_async_remote_copy(
            piece(block, c), piece(block, c), sem, held_recv.at[c, block],
            device_id=to, device_id_type=MESH,
        )

    def core_copy(block, c):
        return pltpu.make_async_remote_copy(
            piece(block, c), other.at[block, pl.ds(c * sub, sub)], core_send.at[c, block],
            other_recv.at[block], device_id=partner, device_id_type=MESH,
        )

    beside = member(s, 1 - my_a, my_b, s)
    beside_partner = member(s, 1 - my_a, my_b, 1 - s)

    def cross_copy(block, c, sem):
        return pltpu.make_async_remote_copy(
            piece(block, c), other.at[block, pl.ds(c * sub, sub)], sem, other_recv.at[block],
            device_id=beside_partner, device_id_type=MESH,
        )

    def at_b(k):
        return lax.rem(my_b + k, my_n)

    def beyond(k):
        return member(s, my_a, at_b(k), s)

    def arrived(block, c, begin):
        if begin:
            wait_bytes(piece(block, c), held_recv.at[c, block])
            core_copy(block, c).start()
        else:
            core_copy(block, c).wait_send()

    def act_on(kind, c, begin):
        run = lambda copy: copy.start() if begin else copy.wait_send()
        if kind == "P":
            if begin:
                rows = pl.ds(c * sub, sub)
                part_copy(c).wait_recv()
                theirs = from_fixed(fixed_in[rows], units[rows, 0:1])
                raw = (part[rows] + theirs) + xs[
                    pl.ds(own_rows + c * sub, sub)
                ].astype(jnp.float32)
                norms = lax.rsqrt(jnp.sum(raw * raw, axis=-1, keepdims=True) + 1e-06)
                held[mine, rows] = (raw * norms).astype(jnp.bfloat16)
            others(my_n, lambda k: run(held_copy(mine, c, beyond(k), far_send.at[c, k])))
            run(held_copy(mine, c, beside, near_send.at[c]))
            run(core_copy(mine, c))
        elif kind == "A":
            arrived(block_of(1 - my_a, my_b), c, begin)
        elif kind == "B":
            def from_b(k):
                block = block_of(my_a, at_b(k))
                if begin:
                    wait_bytes(piece(block, c), held_recv.at[c, block])
                if c >= DIRECT:
                    run(cross_copy(block, c, cross_send.at[c, k]))
                run(held_copy(block, c, beside, fwd_send.at[c, k]))
                run(core_copy(block, c))

            others(my_n, from_b)
        else:
            def from_both(k):
                block = block_of(1 - my_a, at_b(k))
                if begin:
                    wait_bytes(piece(block, c), held_recv.at[c, block])
                if c < DIRECT:
                    run(core_copy(block, c))

            others(my_n, from_both)

    scale_value, bias_value = scale_ref[...], bias_ref[...]
    width = held.shape[2]
    slot = d * n_tensor + x

    def loss_copy(n):
        return pltpu.make_async_remote_copy(
            loss_row, loss_all.at[slot], loss_send, loss_recv,
            device_id=device_of(n), device_id_type=MESH,
        )

    def send_loss():
        loss_row[...] = jnp.sum(loss_acc[...], axis=0, keepdims=True)
        loss_all[slot] = loss_row[...]

        def body(n, carry):
            loss_copy(lax.rem(me + n, n_all)).start()
            return carry

        lax.fori_loop(1, n_all, body, 0)

    def tile_of(ref, tile):
        return ref[pl.ds(tile * tile_blocks, tile_blocks)].reshape(tile_rows, width)

    def score(tower, a, tile):
        slides, reports = (held, other) if tower == 0 else (other, held)
        logits = scale_value * lax.dot_general(
            slides[pl.ds(a * PAIR, PAIR)].reshape(rows_dp, width), tile_of(reports, tile),
            (((1,), (1,)), ((), ())), preferred_element_type=jnp.float32,
        ) + bias_value
        rows = pl.ds(pl.multiple_of(a * rows_dp, 16), rows_dp)
        shift = tile * (PAIR * INNER * rows_dp)
        for j in range(tile_rows // 128):
            lanes = slice(j * 128, (j + 1) * 128)
            sign = jnp.where(left[rows] == right[:, lanes] + shift, 1.0, -1.0).astype(jnp.float32)
            u = -sign * logits[:, lanes]
            e = jnp.exp(-jnp.abs(u))
            if tower == 1:
                loss_acc[...] += jnp.maximum(u, 0.0) + jnp.log1p(e)
            sigmoid = jnp.where(u >= 0, 1.0, e) / (1.0 + e)
            scores[rows, lanes] = (-scale_value * sign * sigmoid).astype(jnp.bfloat16)

    def slide_terms(a, tile):
        return jnp.dot(
            scores[pl.ds(pl.multiple_of(a * rows_dp, 16), rows_dp)], tile_of(other, tile),
            preferred_element_type=jnp.float32,
        ).reshape(PAIR, own_rows, width)

    def report_terms():
        return lax.dot_general(
            scores[...], tile_of(other, 0), (((0,), (0,)), ((), ())),
            preferred_element_type=jnp.float32,
        ).reshape(tile_blocks, own_rows, width)

    part_rows = own_rows // R_SUB

    def sent_copy(block, c, target, to, sem):
        return pltpu.make_async_remote_copy(
            sent.at[block, pl.ds(c * part_rows, part_rows)], target, sent_send.at[block, c], sem,
            device_id=to, device_id_type=MESH,
        )

    def sent_unit_copy(block, h, target, to, sem):
        return pltpu.make_async_remote_copy(
            sent_unit.at[block, h], target, sent_unit_send.at[block, h], sem,
            device_id=to, device_id_type=MESH,
        )

    def owner_unit_copy(block, h, a, b):
        return sent_unit_copy(
            block, h, got_unit.at[s, my_b], member(s, a, b, h), got_unit_recv.at[s, my_b]
        )

    def owner_copy(block, c, a, b):
        per = R_SUB // n_section
        return sent_copy(
            block, c, got.at[s, my_b, pl.ds(c % per * part_rows, part_rows)], member(s, a, b, c // per),
            got_recv.at[s, my_b],
        )

    def halves_to_rows(block, units_of):
        for h in range(n_section):
            sent_unit[block, h] = to_row(units_of[h * quarter:(h + 1) * quarter])

    def send_across(k, begin):
        b = at_b(k)
        block = block_of(1 - my_a, b)
        copies = [sent_unit_copy(block, 0, relay_unit.at[b], beside, relay_unit_recv.at[b])]
        copies += [
            sent_copy(block, c, relay.at[b, pl.ds(c * part_rows, part_rows)], beside, relay_recv.at[b, c])
            for c in range(R_SUB)
        ]
        if begin:
            values, units_of = to_fixed(grad[block])
            sent[block] = values
            sent_unit[block, 0] = to_row(units_of)
        for copy in copies:
            copy.start() if begin else copy.wait_send()

    def send_beside(begin):
        block = block_of(1 - my_a, my_b)
        if begin:
            values, units_of = to_fixed(grad[block])
            sent[block] = values
            halves_to_rows(block, units_of)
        for h in range(n_section):
            copy = owner_unit_copy(block, h, 1 - my_a, my_b)
            copy.start() if begin else copy.wait_send()
        for c in range(R_SUB):
            copy = owner_copy(block, c, 1 - my_a, my_b)
            copy.start() if begin else copy.wait_send()

    def pass_on(k, begin):
        b = at_b(k)
        block = block_of(my_a, b)
        if begin:
            top = jnp.max(jnp.abs(grad[block]), axis=-1, keepdims=True)
            wait_bytes(relay_unit.at[b], relay_unit_recv.at[b])
            came = to_column(relay_unit[b], own_rows)
            units_of = jnp.maximum(top, 1e-30) * (1.0 / TOP) + came
            halves_to_rows(block, units_of)
            inverse = 1.0 / units_of
        for h in range(n_section):
            copy = owner_unit_copy(block, h, my_a, b)
            copy.start() if begin else copy.wait_send()
        for c in range(R_SUB):
            if begin:
                rows = slice(c * part_rows, (c + 1) * part_rows)
                wait_bytes(relay.at[b, pl.ds(c * part_rows, part_rows)], relay_recv.at[b, c])
                value = grad[block, rows] + from_fixed(relay[b, rows], came[rows])
                sent[block, rows] = jnp.round(value * inverse[rows]).astype(jnp.int32).astype(jnp.int16)
            copy = owner_copy(block, c, my_a, b)
            copy.start() if begin else copy.wait_send()

    twin_copy = pltpu.make_async_remote_copy(
        grad.at[mine, pl.ds(pl.multiple_of((1 - s) * quarter, 16), quarter)], twin,
        twin_send, twin_recv, device_id=partner, device_id_type=MESH,
    )

    def other_block(block):
        wait_bytes(other.at[block], other_recv.at[block])

    def make_ids():
        right[...] = report_ids(iota((1, tile_rows), 1))
        pair_copy.wait_recv()
        for b in range(PAIR):
            column = to_column(pairs[b].astype(jnp.float32), rows_dp).astype(jnp.int32)
            for a in range(n_tensor):
                at = (a * PAIR + b) * own_rows
                left[at:at + own_rows] = jnp.broadcast_to(
                    column[a * own_rows:(a + 1) * own_rows], (own_rows, 128)
                )

    def run_tower(tower):
        for kind, c in events(tower):
            act_on(kind, c, True)
            if (kind, c) == ("P", N_SUB - 1):
                make_ids()
        if n_tiles > 1:
            def wait_block(block, carry):
                other_block(block)
                return carry

            lax.fori_loop(0, 2 * (n_near if tower == 0 else PAIR), wait_block, 0)
            if tower == 0:
                grad[0:tile_blocks] = jnp.zeros_like(grad[0:tile_blocks])

            def tile_step(tile, carry):
                for a in range(2):
                    score(tower, a, tile)
                    if tower == 0:
                        grad[a * PAIR:(a + 1) * PAIR] += slide_terms(a, tile)
                if tower == 1:
                    grad[pl.ds(tile * tile_blocks, tile_blocks)] = report_terms()
                return carry

            lax.fori_loop(0, n_tiles, tile_step, 0)
            others(my_n, lambda k: send_across(k, True))
            send_beside(True)
        elif tower == 0:
            for block in range(tile_blocks):
                other_block(block)
            score(tower, 1 - my_a, 0)
            grad[pl.ds((1 - my_a) * PAIR, PAIR)] = slide_terms(1 - my_a, 0)
            send_across(1, True)
            send_beside(True)
            score(tower, my_a, 0)
            grad[pl.ds(my_a * PAIR, PAIR)] = slide_terms(my_a, 0)
        else:
            for a in (x, 1 - x):
                for b in (far, 1 - far):
                    other_block(block_of(a, b))
                score(tower, a, 0)
            grad[...] = report_terms()
            send_across(1, True)
            send_beside(True)
        twin_copy.start()
        if tower == 1:
            send_loss()
        others(my_n, lambda k: pass_on(k, True))

    for tower in range(n_section):
        @pl.when(s == tower)
        def _():
            run_tower(tower)

    def add_got(t, b, out):
        wait_bytes(got_unit.at[t, b], got_unit_recv.at[t, b])
        wait_bytes(got.at[t, b], got_recv.at[t, b])
        out[...] += from_fixed(got[t, b], to_column(got_unit[t, b], quarter))

    def collect(t, out):
        _, b, count = place_of(t)
        add_got(t, b, out)
        others(count, lambda k: add_got(t, lax.rem(b + k, count), out))

    mine_out[...] = grad[mine, pl.ds(pl.multiple_of(s * quarter, 16), quarter)]
    twin_copy.wait_recv()
    theirs_out[...] = twin[...]
    collect(s, mine_out)
    collect(1 - s, theirs_out)
    for c in range(N_SUB):
        part_copy(c).wait_send()
    unit_copy.wait_send()
    pair_copy.wait_send()
    for kind, c in events(0):
        act_on(kind, c, False)
    others(my_n, lambda k: send_across(k, False))
    send_beside(False)
    others(my_n, lambda k: pass_on(k, False))
    twin_copy.wait_send()
    n_chips = n_dp * n_tensor

    @pl.when(s == 1)
    def _():
        wait_bytes(loss_all.at[pl.ds(0, n_all - 1)], loss_send)
        wait_bytes(loss_all.at[pl.ds(0, n_chips - 1)], loss_recv)

    @pl.when(s != 1)
    def _():
        wait_bytes(loss_all.at[pl.ds(0, n_chips)], loss_recv)

    loss_out[...] = jnp.broadcast_to(jnp.sum(loss_all[0:n_chips]) / total, loss_out.shape)


def local(tower_input, up_weight, down_weight, pair, scale, bias):
    n_dp = lax.axis_size("dp")
    n_section = lax.axis_size("section")
    n_tensor = lax.axis_size("tensor")
    inputs, up_w, down_w = tower_input[0], up_weight[0], down_weight[0]
    rows, width = inputs.shape
    hidden = up_w.shape[1]
    group = n_section * n_tensor
    quarter = rows // group
    own_rows = n_section * quarter
    total = n_dp * rows
    n_near = n_dp // (INNER * PAIR)
    blocks = 2 * n_near
    tile_rows = 2 * PAIR * own_rows

    f32, bf16, i16, i32 = jnp.float32, jnp.bfloat16, jnp.int16, jnp.int32
    vmem = pl.BlockSpec(memory_space=pltpu.VMEM)
    hbm = pl.BlockSpec(memory_space=pl.ANY)
    dma = pltpu.SemaphoreType.DMA
    n_all = n_dp * group
    dims = (n_dp, n_section, n_tensor, n_near, total)
    loss, mine, theirs = pl.pallas_call(
        functools.partial(kernel, dims),
        out_shape=(
            jax.ShapeDtypeStruct((1, 128), f32),
            jax.ShapeDtypeStruct((quarter, width), f32),
            jax.ShapeDtypeStruct((quarter, width), f32),
        ),
        in_specs=[hbm] * 6,
        out_specs=(vmem, vmem, vmem),
        scratch_shapes=[
            pltpu.VMEM((rows, width), bf16),
            pltpu.VMEM((width, hidden), bf16),
            pltpu.VMEM((hidden, width), bf16),
            pltpu.VMEM((rows, hidden), bf16),
            pltpu.VMEM((own_rows, width), f32),
            pltpu.VMEM((own_rows, width), i16),
            pltpu.VMEM((own_rows, width), i16),
            pltpu.VMEM((1, 128), f32),
            pltpu.VMEM((1, 128), f32),
            pltpu.VMEM((own_rows, 128), f32),
            pltpu.VMEM((PAIR, 1, rows), i32),
            pltpu.VMEM((tile_rows, 128), i32),
            pltpu.VMEM((1, tile_rows), i32),
            pltpu.VMEM((blocks, own_rows, width), bf16),
            pltpu.VMEM((blocks, own_rows, width), bf16),
            pltpu.VMEM((tile_rows, tile_rows), bf16),
            pltpu.VMEM((blocks, own_rows, width), f32),
            pltpu.VMEM((blocks, own_rows, width), i16),
            pltpu.VMEM((blocks, n_section, 1, 128), f32),
            pltpu.VMEM((n_near, own_rows, width), i16),
            pltpu.VMEM((n_near, 1, 128), f32),
            pltpu.VMEM((n_section, n_near, quarter, width), i16),
            pltpu.VMEM((n_section, n_near, 1, 128), f32),
            pltpu.VMEM((quarter, width), f32),
            pltpu.VMEM((rows, 128), f32),
            pltpu.VMEM((1, 128), f32),
            pltpu.VMEM((n_all, 1, 128), f32),
            pltpu.VMEM((1, 1), f32),
            pltpu.VMEM((1, 1), f32),
            pltpu.VMEM((1, rows), i32),
            dma((3,)),
            dma((group,)),
            dma((UP_PARTS,)),
            dma((DOWN_PARTS,)),
            dma((N_SUB,)),
            dma((N_SUB,)),
            dma, dma, dma, dma,
            dma((N_SUB, blocks)),
            dma((N_SUB,)),
            dma((N_SUB, n_near)),
            dma((N_SUB, n_near)),
            dma((N_SUB, n_near)),
            dma((N_SUB, blocks)),
            dma((blocks,)),
            dma((blocks, R_SUB)),
            dma((blocks, n_section)),
            dma((n_near, R_SUB)),
            dma((n_near,)),
            dma((n_section, n_near)),
            dma((n_section, n_near)),
            dma, dma, dma, dma,
        ],
        compiler_params=pltpu.CompilerParams(
            collective_id=0, has_side_effects=True, vmem_limit_bytes=52 * 1024 * 1024
        ),
    )(scale.reshape(1, 1), bias.reshape(1, 1), *(
        pltpu.with_memory_space_constraint(a, pltpu.HBM)
        for a in (pair.reshape(1, rows), inputs, up_w, down_w)
    ))
    first_core = lax.axis_index("section") == 0
    return (
        loss[0, :1],
        jnp.where(first_core, mine, theirs),
        jnp.where(first_core, theirs, mine),
    )


def solution(mesh):
    return jax.shard_map(
        local,
        mesh=mesh,
        in_specs=(
            P("section", "dp", None),
            P("section", None, "tensor"),
            P("section", "tensor", None),
            P("dp"),
            P(),
            P(),
        ),
        out_specs=(P(), P(("dp", "section", "tensor"), None), P(("dp", "section", "tensor"), None)),
        check_vma=False,
    )
```
